256 devices in a mesh: groups: 2 (over y), patch: 16 (over z), cfg: 2 (over core), head: 4 (over x).
Axes of the slice: x: 4, y: 2, z: 16, core: 2. Of those that a mesh axis runs over, the one named last changes fastest.
The devices are a block of a 4x16x16 slice.
Arguments:
- img_hidden: bfloat16 [2, 8192, 3072], P('cfg', ('groups', 'patch')), parts along dimension 1, may hold values from -40 to 40
- txt_hidden: bfloat16 [2, 512, 3072], P('cfg', ('groups', 'patch')), parts along dimension 1, may hold values from -6 to 6
- modulation: float32 [4, 3, 3072], P(('groups', 'cfg')), parts along dimension 0, may hold values from -4 to 4
- w_qkv: bfloat16 [3072, 3, 1536], P(None, None, 'head'), may hold values from -0.109375 to 0.109375
- q_gain: float32 [128], replicated, may hold values from 1.2 to 2.5
- k_gain: float32 [128], replicated, may hold values from 1.2 to 2.5
- w_out: bfloat16 [1536, 3072], P('head'), may hold values from -0.15625 to 0.15625
- b_out: float32 [3072], replicated, may hold values from -3 to 3
- stale_kv: bfloat16 [2, 2, 8704, 1536], P('cfg', None, ('groups', 'patch'), 'head'), parts along dimension 2, may hold values from -500 to 500
- final_mod: float32 [4, 2, 3072], P(('groups', 'cfg')), parts along dimension 0, may hold values from -3 to 3
- w_final: bfloat16 [3072, 64], replicated, may hold values from -0.109375 to 0.109375
- b_final: float32 [64], replicated, may hold values from -3 to 3
- latent: float32 [8192, 64], P(('groups', 'patch', 'cfg', 'head')), parts along dimension 0, may hold values from -6 to 6
- prev_denoised: float32 [8192, 64], P(('groups', 'patch', 'cfg', 'head')), parts along dimension 0, may hold values from -24 to 24
- guidance: float32 [2], P('groups'), parts along dimension 0, may hold values from 2 to 5
- step_index: int32 [1], replicated, may hold values from 14 to 21
- step_count: int32 [1], replicated, may hold values from 24 to 27
Outputs:
- fresh_kv: bfloat16 [2, 2, 8704, 1536], P('cfg', None, ('groups', 'patch'), 'head'), parts along dimension 2
- next_latent: float32 [8192, 64], P(('groups', 'patch', 'cfg', 'head')), parts along dimension 0
- denoised: float32 [8192, 64], P(('groups', 'patch', 'cfg', 'head')), parts along dimension 0
The draws below stay inside these ranges and needn't reach their ends.
There are 2 independent parts, one for each index of `groups`. The reference program is written for one: setup_inputs(seed, part) draws one part's arguments, and reference() takes and returns one part's arrays. A program takes and returns all parts, laid end to end along the dimension named above; an argument that names none is the same for every part. Nothing has to cross between parts.
All inputs are finite; a program needn't handle non-finite values.
Results may differ from the reference program's by a relative error of at most 0.0075.
The reference program's roundings to bfloat16 on the way (of `weights`, `attn` and `final_in`) count: a program that leaves them out, or rounds other values in their place, can miss the bound.
Values may be sent and summed in bfloat16 or wider, within the bound.
No kernel may reach another device: no remote copies, remote signals or barrier semaphores. Data moves between devices by JAX's collectives and lax.ppermute only.
A program may use at most 128 MiB of HBM per device.

```python
import math
import jax
import jax.numpy as jnp
from jax import lax

D = 3072
HD = 128
CH = 64
HEADS = 12
GRID_W = 128
IMG_DEV = 256
TXT_DEV = 16
IMG = 4096
TXT = 256
KV_DEV = 272
KVTOK = 4352
N_PATCH = 16


def draw_img_hidden(key, part):
    key_base = jax.random.fold_in(key, 0)
    values = jax.random.normal(key_base, (2, IMG, D), jnp.float32)
    return jnp.clip(values, -40.0, 40.0).astype(jnp.bfloat16)


def draw_stale_kv(key, part):
    key_base = jax.random.fold_in(key, 0)
    width = HEADS * HD
    values = jax.random.normal(key_base, (2, 2, KVTOK, width), jnp.float32)
    values = values * jnp.array([1.5, 1.0], jnp.float32).reshape(1, 2, 1, 1)
    return jnp.clip(values, -500.0, 500.0).astype(jnp.bfloat16)


def shard_levels(stream_key, shape, cuts, low, high):
    def one(axis_at, shards_of):
        steps = jax.random.uniform(jax.random.fold_in(jax.random.fold_in(stream_key, 6), axis_at), (shards_of,), jnp.float32, low / len(cuts), high / len(cuts))
        return jnp.repeat(jnp.exp(steps), shape[axis_at] // shards_of).reshape((-1,) + (1,) * (len(shape) - axis_at - 1))

    loudness = one(*cuts[0])
    for cut in cuts[1:]:
        loudness = loudness * one(*cut)
    return loudness


def normal_values(rng, extent, deviation, limit, shards=(), held_as=jnp.bfloat16):
    drawn = deviation * jax.random.normal(rng, extent, jnp.float32)
    if shards:
        drawn = drawn * shard_levels(rng, extent, shards, -0.22, 0.18)
    return jnp.clip(drawn, -limit, limit).astype(held_as)


def setup_inputs(seed: int = 0, part: int = 0) -> dict:
    splits = jax.random.split(jax.random.key(seed), 18)
    part_splits = jax.random.split(jax.random.fold_in(splits[17], part), 18)
    img_hidden = draw_img_hidden(jax.random.fold_in(jax.random.fold_in(splits[17], part), 71), part)
    txt_hidden = normal_values(part_splits[1], (2, TXT, D), 1.0, 6.0, ((0, 2), (1, 16)))
    modulation = normal_values(part_splits[2], (2, 3, D), 0.7, 4.0, ((0, 2),), jnp.float32)
    w_qkv = normal_values(splits[3], (D, 3, HEADS * HD), D ** -0.5, 0.109375, ((2, 4),))
    q_gain = jnp.clip(jnp.exp(jax.random.uniform(splits[4], (HD,), jnp.float32, math.log(1.2), math.log(2.5))), 1.2, 2.5)
    k_gain = jnp.clip(jnp.exp(jax.random.uniform(splits[5], (HD,), jnp.float32, math.log(1.2), math.log(2.5))), 1.2, 2.5)
    w_out = normal_values(splits[6], (HEADS * HD, D), (HEADS * HD) ** -0.5, 0.15625, ((0, 4),))
    b_out = normal_values(splits[7], (D,), 0.5, 3.0, (), jnp.float32)
    stale_kv = draw_stale_kv(jax.random.fold_in(jax.random.fold_in(splits[17], part), 71), part)
    final_mod = normal_values(part_splits[9], (2, 2, D), 0.5, 3.0, ((0, 2),), jnp.float32)
    w_final = normal_values(splits[10], (D, CH), D ** -0.5, 0.109375)
    b_final = normal_values(splits[11], (CH,), 0.5, 3.0, (), jnp.float32)
    latent = normal_values(part_splits[12], (IMG, CH), 1.0, 6.0, ((0, 128),), jnp.float32)
    prev_denoised = normal_values(part_splits[13], (IMG, CH), 4.0, 24.0, ((0, 128),), jnp.float32)
    guidance = jnp.clip(jax.random.uniform(part_splits[14], (1,), jnp.float32, 2.0, 5.0), 2.0, 5.0)
    step_index = jax.random.randint(splits[15], (1,), 14, 22).astype(jnp.int32)
    step_count = jax.random.randint(splits[16], (1,), 24, 28).astype(jnp.int32)
    return dict(img_hidden=img_hidden, txt_hidden=txt_hidden, modulation=modulation, w_qkv=w_qkv, q_gain=q_gain, k_gain=k_gain, w_out=w_out, b_out=b_out, stale_kv=stale_kv, final_mod=final_mod, w_final=w_final, b_final=b_final, latent=latent, prev_denoised=prev_denoised, guidance=guidance, step_index=step_index, step_count=step_count)


epsilon = 1e-06
time_shift = 3.0

def layer_norm(values):
    mean_val = lax.optimization_barrier(jnp.mean(values, axis=-1, keepdims=True))
    centered = values - mean_val
    variance = lax.optimization_barrier(jnp.mean(centered * centered, axis=-1, keepdims=True))
    return centered * lax.rsqrt(variance + epsilon)

def rms_norm(values, gain_vec):
    return values * lax.rsqrt(lax.optimization_barrier(jnp.mean(values * values, axis=-1, keepdims=True)) + epsilon) * gain_vec

def rotate(values, positions, grid_width):
    quarter = values.shape[-1] // 4
    freqs = 10000.0 ** (-jnp.arange(quarter, dtype=jnp.float32) / quarter)
    row_pos = (positions // grid_width).astype(jnp.float32)
    col_pos = (positions % grid_width).astype(jnp.float32)
    angles = jnp.stack([row_pos[:, None] * freqs[None, :], col_pos[:, None] * freqs[None, :]], axis=1)
    cosine = jnp.cos(angles)[:, None]
    sine = jnp.sin(angles)[:, None]
    shaped = values.reshape(values.shape[0], values.shape[1], 2, 2, quarter)
    first = shaped[:, :, :, 0]
    second = shaped[:, :, :, 1]
    turned = jnp.stack([first * cosine - second * sine, second * cosine + first * sine], axis=3)
    return turned.reshape(values.shape)

def noise_level(index, count):
    frac = 1.0 - index / count
    lift = math.exp(time_shift)
    return lift * frac / (lift * frac + 1.0 - frac)

def log_ratio(sigma_val):
    return jnp.log(1.0 - sigma_val) - jnp.log(sigma_val)

def solver_step(cond, uncond, guidance, step_index, step_count, latent, prev_denoised):
    guided = uncond + guidance[0] * (cond - uncond)
    index = step_index[0].astype(jnp.float32)
    count = step_count[0].astype(jnp.float32)
    sigma_prev = noise_level(index - 1.0, count)
    sigma_now = noise_level(index, count)
    sigma_next = noise_level(index + 1.0, count)
    step_now = log_ratio(sigma_next) - log_ratio(sigma_now)
    step_prev = log_ratio(sigma_now) - log_ratio(sigma_prev)
    ratio = step_prev / step_now
    denoised = latent - sigma_now * guided
    blend = (1.0 + 0.5 / ratio) * denoised - 0.5 / ratio * prev_denoised
    next_latent = sigma_next / sigma_now * latent - (1.0 - sigma_next) * (jnp.exp(-step_now) - 1.0) * blend
    return (next_latent, denoised)

def reference(img_hidden, txt_hidden, modulation, w_qkv, q_gain, k_gain, w_out, b_out, stale_kv, final_mod, w_final, b_final, latent, prev_denoised, guidance, step_index, step_count):
    inv_root = HD ** (-0.5)
    head_width = HEADS * HD
    weight_flat = w_qkv.reshape(D, 3 * head_width)
    positions = jnp.arange(IMG, dtype=jnp.int32)
    fresh_list = []
    velocities = []
    for branch in range(2):
        shift_vec = modulation[branch, 0]
        scale_vec = modulation[branch, 1]
        gate_vec = modulation[branch, 2]
        modded_img = (layer_norm(img_hidden[branch].astype(jnp.float32)) * (1.0 + scale_vec) + shift_vec).astype(jnp.bfloat16)
        modded_txt = (layer_norm(txt_hidden[branch].astype(jnp.float32)) * (1.0 + scale_vec) + shift_vec).astype(jnp.bfloat16)
        proj_img = jnp.dot(modded_img, weight_flat, preferred_element_type=jnp.float32).reshape(IMG, 3, HEADS, HD)
        proj_txt = jnp.dot(modded_txt, weight_flat, preferred_element_type=jnp.float32).reshape(TXT, 3, HEADS, HD)
        queries = lax.optimization_barrier(rotate(rms_norm(proj_img[:, 0], q_gain), positions, GRID_W).astype(jnp.bfloat16))
        img_keys = rotate(rms_norm(proj_img[:, 1], k_gain), positions, GRID_W).astype(jnp.bfloat16)
        img_vals = proj_img[:, 2].astype(jnp.bfloat16)
        txt_keys = rms_norm(proj_txt[:, 1], k_gain).astype(jnp.bfloat16)
        txt_vals = proj_txt[:, 2].astype(jnp.bfloat16)

        def joined(txt_part, img_part):
            return jnp.concatenate([txt_part.reshape(N_PATCH, TXT_DEV, HEADS, HD), img_part.reshape(N_PATCH, IMG_DEV, HEADS, HD)], axis=1).reshape(KVTOK, HEADS, HD)
        fresh_keys = lax.optimization_barrier(joined(txt_keys, img_keys))
        fresh_vals = lax.optimization_barrier(joined(txt_vals, img_vals))
        fresh_list.append(jnp.stack([fresh_keys.reshape(KVTOK, head_width), fresh_vals.reshape(KVTOK, head_width)]))
        stale_keys = stale_kv[branch, 0].reshape(KVTOK, HEADS, HD)
        stale_vals = stale_kv[branch, 1].reshape(KVTOK, HEADS, HD)

        def attend(block):
            query_blk = lax.dynamic_slice_in_dim(queries, block * IMG_DEV, IMG_DEV, 0)
            own_keys = lax.dynamic_slice_in_dim(fresh_keys, block * KV_DEV, KV_DEV, 0)
            own_vals = lax.dynamic_slice_in_dim(fresh_vals, block * KV_DEV, KV_DEV, 0)
            keys_all = lax.dynamic_update_slice_in_dim(stale_keys, own_keys, block * KV_DEV, 0)
            vals_all = lax.dynamic_update_slice_in_dim(stale_vals, own_vals, block * KV_DEV, 0)
            scores = jnp.einsum('qhd,khd->hqk', query_blk.astype(jnp.float32), keys_all.astype(jnp.float32)) * inv_root
            top = lax.optimization_barrier(jnp.max(scores, axis=-1, keepdims=True))
            expo = jnp.exp(scores - top)
            denom = lax.optimization_barrier(jnp.sum(expo, axis=-1))
            weights = lax.optimization_barrier(expo.astype(jnp.bfloat16))
            weighted = jnp.einsum('hqk,khd->hqd', weights.astype(jnp.float32), vals_all.astype(jnp.float32))
            attn_blk = weighted / denom[..., None]
            return attn_blk.transpose(1, 0, 2).reshape(IMG_DEV, head_width).astype(jnp.bfloat16)
        attn = lax.map(attend, jnp.arange(N_PATCH, dtype=jnp.int32)).reshape(IMG, head_width)
        projected = jnp.dot(attn, w_out, preferred_element_type=jnp.float32)
        mixed = img_hidden[branch].astype(jnp.float32) + gate_vec * (projected + b_out)
        final_in = (layer_norm(mixed) * (1.0 + final_mod[branch, 1]) + final_mod[branch, 0]).astype(jnp.bfloat16)
        velocities.append(jnp.dot(final_in, w_final, preferred_element_type=jnp.float32) + b_final)
    next_latent, denoised = solver_step(velocities[0], velocities[1], guidance, step_index, step_count, latent, prev_denoised)
    return (jnp.stack(fresh_list), next_latent, denoised)
```

```python
import math

import jax
import jax.numpy as jnp
from jax import lax
from jax.experimental import pallas as pl
from jax.experimental.pallas import tpu as pltpu
from jax.sharding import PartitionSpec as P

D = 3072
HD = 128
CH = 64
GRID_W = 128


epsilon = 1e-06
time_shift = 3.0


def layer_norm(values):
    mean_val = jnp.mean(values, axis=-1, keepdims=True)
    centered = values - mean_val
    variance = jnp.mean(centered * centered, axis=-1, keepdims=True)
    return centered * lax.rsqrt(variance + epsilon)


def rms_norm(values, gain_vec):
    return (
        values * lax.rsqrt(jnp.mean(values * values, axis=-1, keepdims=True) + epsilon) * gain_vec
    )


def rotate(values, positions, grid_width):
    quarter = values.shape[-1] // 4
    freqs = 10000.0 ** (-jnp.arange(quarter, dtype=jnp.float32) / quarter)
    row_pos = (positions // grid_width).astype(jnp.float32)
    col_pos = (positions % grid_width).astype(jnp.float32)
    angles = jnp.stack(
        [row_pos[:, None] * freqs[None, :], col_pos[:, None] * freqs[None, :]], axis=1
    )
    cosine = jnp.cos(angles)[:, None]
    sine = jnp.sin(angles)[:, None]
    shaped = values.reshape(values.shape[0], values.shape[1], 2, 2, quarter)
    first = shaped[:, :, :, 0]
    second = shaped[:, :, :, 1]
    turned = jnp.stack([first * cosine - second * sine, second * cosine + first * sine], axis=3)
    return turned.reshape(values.shape)


def noise_level(index, count):
    frac = 1.0 - index / count
    lift = math.exp(time_shift)
    return lift * frac / (lift * frac + 1.0 - frac)


def log_ratio(sigma_val):
    return jnp.log(1.0 - sigma_val) - jnp.log(sigma_val)


def solver_scalars(guidance, step_index, step_count):
    index = step_index[0].astype(jnp.float32)
    count = step_count[0].astype(jnp.float32)
    sigma_prev = noise_level(index - 1.0, count)
    sigma_now = noise_level(index, count)
    sigma_next = noise_level(index + 1.0, count)
    step_now = log_ratio(sigma_next) - log_ratio(sigma_now)
    step_prev = log_ratio(sigma_now) - log_ratio(sigma_prev)
    ratio = step_prev / step_now
    return jnp.stack(
        [
            guidance[0],
            sigma_now,
            1.0 + 0.5 / ratio,
            0.5 / ratio,
            sigma_next / sigma_now,
            (1.0 - sigma_next) * (jnp.exp(-step_now) - 1.0),
        ]
    )


def attend_kernel(where, q_ref, fresh_ref, gathered_ref, out_ref, keys, vals, key_sem, val_sem):
    blocks, _, kv_rows, width = gathered_ref.shape
    heads = width // HD
    mine = where[0]
    for index, (held, sem) in enumerate(((keys, key_sem), (vals, val_sem))):
        for block in range(blocks):

            @pl.when(mine == block)
            def _():
                pltpu.make_async_copy(fresh_ref.at[index], held.at[block], sem.at[block]).start()

            @pl.when(mine != block)
            def _():
                pltpu.make_async_copy(
                    gathered_ref.at[block, index], held.at[block], sem.at[block]
                ).start()

    def arrived(held, sem):
        for block in range(blocks):
            pltpu.make_async_copy(fresh_ref.at[0], held.at[block], sem.at[block]).wait()

    scale = math.log2(math.e) * HD ** (-0.5)
    total_keys = blocks * kv_rows
    arrived(keys, key_sem)
    for head in range(heads):
        lanes = pl.ds(head * HD, HD)
        key_mat = keys[:, :, lanes].reshape(total_keys, HD)
        scores = lax.dot_general(
            q_ref[:, lanes], key_mat, (((1,), (1,)), ((), ())), preferred_element_type=jnp.float32
        )
        top = jnp.max(scores, axis=-1, keepdims=True)
        expo = jnp.exp2(scores * scale - top * scale)
        denom = jnp.sum(expo, axis=-1, keepdims=True)
        if head == 0:
            arrived(vals, val_sem)
        val_mat = vals[:, :, lanes].reshape(total_keys, HD)
        acc = jnp.dot(expo.astype(jnp.bfloat16), val_mat, preferred_element_type=jnp.float32)
        out_ref[:, lanes] = (acc / denom).astype(jnp.bfloat16)


def attend(queries, fresh, gathered, patch_index):
    rows, width = queries.shape
    blocks, _, kv_rows, _ = gathered.shape
    flops = 4 * rows * blocks * kv_rows * width
    vmem = pl.BlockSpec(memory_space=pltpu.VMEM)
    hbm = pl.BlockSpec(memory_space=pl.ANY)
    return pl.pallas_call(
        attend_kernel,
        out_shape=jax.ShapeDtypeStruct((rows, width), jnp.bfloat16),
        in_specs=[pl.BlockSpec(memory_space=pltpu.SMEM), vmem, hbm, hbm],
        out_specs=vmem,
        scratch_shapes=[
            pltpu.VMEM((blocks, kv_rows, width), jnp.bfloat16),
            pltpu.VMEM((blocks, kv_rows, width), jnp.bfloat16),
            pltpu.SemaphoreType.DMA((blocks,)),
            pltpu.SemaphoreType.DMA((blocks,)),
        ],
        compiler_params=pltpu.CompilerParams(vmem_limit_bytes=40 * 1024 * 1024),
        cost_estimate=pl.CostEstimate(
            flops=flops,
            bytes_accessed=4 * blocks * kv_rows * width,
            transcendentals=rows * blocks * kv_rows * (width // HD),
        ),
        name="attend",
    )(patch_index.reshape(1), queries, fresh, gathered)


def finish_kernel(
    where,
    numbers,
    attn_ref,
    *refs,
):
    weights = refs[:4]
    (
        hidden_ref,
        gate_ref,
        shift_ref,
        scale_ref,
        b_out_ref,
        w_final_ref,
        b_final_ref,
        prev_ref,
        latent_ref,
        next_ref,
        denoised_ref,
    ) = refs[4:]
    rows = latent_ref.shape[0]
    here = where[0]
    peers = len(weights)

    def of_both(vec_ref):
        return jnp.concatenate(
            [jnp.broadcast_to(vec_ref[b], (rows, vec_ref.shape[-1])) for b in range(2)], axis=0
        )

    projected = None
    for shift, w_ref in enumerate(weights):
        source = lax.rem(here + peers - shift, peers)
        left = jnp.concatenate([attn_ref[b, source] for b in range(2)], axis=0)
        term = jnp.dot(left, w_ref[...], preferred_element_type=jnp.float32)
        projected = term if projected is None else projected + term
    mixed = hidden_ref[...].astype(jnp.float32) + of_both(gate_ref) * (projected + b_out_ref[...])
    normed = layer_norm(mixed)
    final_in = (normed * (1.0 + of_both(scale_ref)) + of_both(shift_ref)).astype(jnp.bfloat16)
    velocity = (
        jnp.dot(final_in, w_final_ref[...], preferred_element_type=jnp.float32) + b_final_ref[...]
    )
    cond = velocity[:rows]
    uncond = velocity[rows:]
    guided = uncond + numbers[0] * (cond - uncond)
    latent = latent_ref[...]
    denoised = latent - numbers[1] * guided
    blend = numbers[2] * denoised - numbers[3] * prev_ref[...]
    denoised_ref[...] = denoised
    next_ref[...] = numbers[4] * latent - numbers[5] * blend


def finish(where, numbers, attn, weights, *rest):
    latent = rest[-1]
    out = jax.ShapeDtypeStruct(latent.shape, jnp.float32)
    smem = pl.BlockSpec(memory_space=pltpu.SMEM)
    vmem = pl.BlockSpec(memory_space=pltpu.VMEM)
    depth = sum(w.shape[0] for w in weights)
    return pl.pallas_call(
        finish_kernel,
        out_shape=(out, out),
        in_specs=[smem, smem] + [vmem] * (1 + len(weights) + len(rest)),
        out_specs=(vmem, vmem),
        compiler_params=pltpu.CompilerParams(vmem_limit_bytes=40 * 1024 * 1024),
        cost_estimate=pl.CostEstimate(
            flops=4 * latent.shape[0] * depth * D,
            bytes_accessed=2 * depth * D,
            transcendentals=0,
        ),
        name="finish",
    )(where, numbers, attn, *weights, *rest)


def body(
    img_hidden,
    txt_hidden,
    modulation,
    w_qkv,
    q_gain,
    k_gain,
    w_out,
    b_out,
    stale_kv,
    final_mod,
    w_final,
    b_final,
    latent,
    prev_denoised,
    guidance,
    step_index,
    step_count,
):
    head_width = w_out.shape[0]
    head_count = head_width // HD
    img_rows = img_hidden.shape[1]
    txt_rows = txt_hidden.shape[1]
    kv_rows = img_rows + txt_rows
    out_rows = latent.shape[0]
    patch_index = lax.axis_index("patch")
    cfg_index = lax.axis_index("cfg")
    head_index = lax.axis_index("head")
    head_total = lax.axis_size("head")

    gathered = lax.all_gather(
        stale_kv.reshape(2 * kv_rows, head_width), "patch", axis=0, tiled=False
    ).reshape(-1, 2, kv_rows, head_width)

    weights = [w_out] + [
        lax.ppermute(w_out, "head", [(i, (i + shift) % head_total) for i in range(head_total)])
        for shift in range(1, head_total)
    ]
    swap = [(0, 1), (1, 0)]
    hidden_rows = img_hidden.reshape(2, head_total, out_rows, D)
    hidden_mine = lax.dynamic_index_in_dim(hidden_rows, head_index, 1, keepdims=False)
    own_hidden = lax.dynamic_index_in_dim(hidden_mine, cfg_index, 0, keepdims=False)
    sent_hidden = lax.dynamic_index_in_dim(hidden_mine, 1 - cfg_index, 0, keepdims=False)
    other_hidden = lax.ppermute(sent_hidden, "cfg", swap)
    own_vecs = jnp.concatenate([modulation[0, 2:], final_mod[0]], axis=0)
    other_vecs = lax.ppermute(own_vecs, "cfg", swap)
    first = cfg_index == 0
    hidden = jnp.concatenate(
        [
            jnp.where(first, own_hidden, other_hidden),
            jnp.where(first, other_hidden, own_hidden),
        ],
        axis=0,
    )
    vecs = jnp.stack(
        [jnp.where(first, own_vecs, other_vecs), jnp.where(first, other_vecs, own_vecs)], axis=0
    )
    numbers = solver_scalars(guidance, step_index, step_count)

    shift_vec = modulation[0, 0]
    scale_vec = modulation[0, 1]
    modded_img = (
        layer_norm(img_hidden[0].astype(jnp.float32)) * (1.0 + scale_vec) + shift_vec
    ).astype(jnp.bfloat16)
    modded_txt = (
        layer_norm(txt_hidden[0].astype(jnp.float32)) * (1.0 + scale_vec) + shift_vec
    ).astype(jnp.bfloat16)
    weight_flat = w_qkv.reshape(D, 3 * head_width)
    proj_img = jnp.dot(modded_img, weight_flat, preferred_element_type=jnp.float32).reshape(
        img_rows, 3, head_count, HD
    )
    proj_txt = jnp.dot(modded_txt, weight_flat, preferred_element_type=jnp.float32).reshape(
        txt_rows, 3, head_count, HD
    )
    positions = patch_index * img_rows + jnp.arange(img_rows, dtype=jnp.int32)
    queries = rotate(rms_norm(proj_img[:, 0], q_gain), positions, GRID_W).astype(jnp.bfloat16)
    img_keys = rotate(rms_norm(proj_img[:, 1], k_gain), positions, GRID_W).astype(jnp.bfloat16)
    img_vals = proj_img[:, 2].astype(jnp.bfloat16)
    txt_keys = rms_norm(proj_txt[:, 1], k_gain).astype(jnp.bfloat16)
    txt_vals = proj_txt[:, 2].astype(jnp.bfloat16)
    fresh_keys = jnp.concatenate([txt_keys, img_keys], axis=0)
    fresh_vals = jnp.concatenate([txt_vals, img_vals], axis=0)
    fresh_kv = jnp.stack(
        [fresh_keys.reshape(kv_rows, head_width), fresh_vals.reshape(kv_rows, head_width)]
    )

    attn = attend(queries.reshape(img_rows, head_width), fresh_kv, gathered, patch_index)
    shared = lax.all_to_all(
        attn.reshape(2 * head_total, out_rows, head_width), ("cfg", "head"), 0, 0, tiled=True
    ).reshape(2, head_total, out_rows, head_width)
    next_latent, denoised = finish(
        head_index.reshape(1),
        numbers,
        shared,
        weights,
        hidden,
        vecs[:, 0:1],
        vecs[:, 1:2],
        vecs[:, 2:3],
        b_out.reshape(1, D),
        w_final,
        b_final.reshape(1, CH),
        prev_denoised,
        latent,
    )
    return (fresh_kv[None], next_latent, denoised)


def solution(mesh):
    return jax.shard_map(
        body,
        mesh=mesh,
        in_specs=(
            P("cfg", ("groups", "patch"), None),
            P("cfg", ("groups", "patch"), None),
            P(("groups", "cfg"), None, None),
            P(None, None, "head"),
            P(),
            P(),
            P("head", None),
            P(),
            P("cfg", None, ("groups", "patch"), "head"),
            P(("groups", "cfg"), None, None),
            P(),
            P(),
            P(("groups", "patch", "cfg", "head"), None),
            P(("groups", "patch", "cfg", "head"), None),
            P("groups"),
            P(),
            P(),
        ),
        out_specs=(
            P("cfg", None, ("groups", "patch"), "head"),
            P(("groups", "patch", "cfg", "head"), None),
            P(("groups", "patch", "cfg", "head"), None),
        ),
        check_vma=False,
    )
```

```python
import functools
import math

import jax
import jax.numpy as jnp
from jax import lax
from jax.experimental import pallas as pl
from jax.experimental.pallas import tpu as pltpu
from jax.sharding import PartitionSpec as P

D = 3072
HD = 128
CH = 64
GRID_W = 128


epsilon = 1e-06
time_shift = 3.0


def layer_norm(values):
    mean_val = jnp.mean(values, axis=-1, keepdims=True)
    centered = values - mean_val
    variance = jnp.mean(centered * centered, axis=-1, keepdims=True)
    return centered * lax.rsqrt(variance + epsilon)


def rms_norm(values, gain_vec):
    return (
        values * lax.rsqrt(jnp.mean(values * values, axis=-1, keepdims=True) + epsilon) * gain_vec
    )


def rotate(values, positions, grid_width):
    quarter = values.shape[-1] // 4
    freqs = 10000.0 ** (-jnp.arange(quarter, dtype=jnp.float32) / quarter)
    row_pos = (positions // grid_width).astype(jnp.float32)
    col_pos = (positions % grid_width).astype(jnp.float32)
    angles = jnp.stack(
        [row_pos[:, None] * freqs[None, :], col_pos[:, None] * freqs[None, :]], axis=1
    )
    cosine = jnp.cos(angles)[:, None]
    sine = jnp.sin(angles)[:, None]
    shaped = values.reshape(values.shape[0], values.shape[1], 2, 2, quarter)
    first = shaped[:, :, :, 0]
    second = shaped[:, :, :, 1]
    turned = jnp.stack([first * cosine - second * sine, second * cosine + first * sine], axis=3)
    return turned.reshape(values.shape)


def noise_level(index, count):
    frac = 1.0 - index / count
    lift = math.exp(time_shift)
    return lift * frac / (lift * frac + 1.0 - frac)


def log_ratio(sigma_val):
    return jnp.log(1.0 - sigma_val) - jnp.log(sigma_val)


def solver_scalars(guidance, step_index, step_count):
    index = step_index[0].astype(jnp.float32)
    count = step_count[0].astype(jnp.float32)
    sigma_prev = noise_level(index - 1.0, count)
    sigma_now = noise_level(index, count)
    sigma_next = noise_level(index + 1.0, count)
    step_now = log_ratio(sigma_next) - log_ratio(sigma_now)
    step_prev = log_ratio(sigma_now) - log_ratio(sigma_prev)
    ratio = step_prev / step_now
    return jnp.stack(
        [
            guidance[0],
            sigma_now,
            1.0 + 0.5 / ratio,
            0.5 / ratio,
            sigma_next / sigma_now,
            (1.0 - sigma_next) * (jnp.exp(-step_now) - 1.0),
        ]
    )


def attend_kernel(first, last, count, *refs):
    q_ref = refs[0]
    blocks = [(refs[1 + 2 * i], refs[2 + 2 * i]) for i in range(count)]
    refs = refs[1 + 2 * count :]
    if not first:
        top_in, denom_in, acc_in = refs[:3]
        refs = refs[3:]
    heads = q_ref.shape[1] // HD
    scale = math.log2(math.e) * HD ** (-0.5)
    def attend_head(head, _):
        lanes = pl.ds(head * HD if last else pl.multiple_of(head * HD, HD), HD)
        query = q_ref[:, lanes]
        scores = [
            lax.dot_general(
                keys[:, lanes], query, (((1,), (1,)), ((), ())), preferred_element_type=jnp.float32
            )
            for keys, _ in blocks
        ]
        top = functools.reduce(jnp.maximum, [jnp.max(s, axis=0, keepdims=True) for s in scores])
        if not first:
            top = jnp.maximum(top, top_in[head])
        shift = top * scale
        denom = None
        acc = None
        for score, (_, vals) in zip(scores, blocks):
            expo = jnp.exp2(score * scale - shift)
            part = jnp.sum(expo, axis=0, keepdims=True)
            term = lax.dot_general(
                vals[:, lanes],
                expo.astype(jnp.bfloat16),
                (((0,), (0,)), ((), ())),
                preferred_element_type=jnp.float32,
            )
            denom = part if denom is None else denom + part
            acc = term if acc is None else acc + term
        if not first:
            factor = jnp.exp2(top_in[head] * scale - shift)
            denom = denom + denom_in[head] * factor
            acc = acc + acc_in[head] * factor
        if last:
            refs[0][:, lanes] = (acc / denom).T.astype(jnp.bfloat16)
        else:
            refs[0][head] = top
            refs[1][head] = denom
            refs[2][head] = acc
        return 0

    if last:
        for head in range(heads):
            attend_head(head, 0)
    else:
        lax.fori_loop(0, heads, attend_head, 0)


def attend(queries, blocks, state, last):
    rows, width = queries.shape
    heads = width // HD
    key_rows = sum(keys.shape[0] for keys, _ in blocks)
    vmem = pl.BlockSpec(memory_space=pltpu.VMEM)
    row = jax.ShapeDtypeStruct((heads, 1, rows), jnp.float32)
    held = (row, row, jax.ShapeDtypeStruct((heads, HD, rows), jnp.float32))
    out_shape = jax.ShapeDtypeStruct((rows, width), jnp.bfloat16) if last else held
    first = state is None
    operands = [queries] + [piece for block in blocks for piece in block]
    operands += [] if first else list(state)
    return pl.pallas_call(
        functools.partial(attend_kernel, first, last, len(blocks)),
        out_shape=out_shape,
        in_specs=[vmem] * len(operands),
        out_specs=vmem if last else (vmem,) * 3,
        compiler_params=pltpu.CompilerParams(vmem_limit_bytes=24 * 1024 * 1024),
        cost_estimate=pl.CostEstimate(
            flops=4 * rows * key_rows * width,
            bytes_accessed=4 * key_rows * width,
            transcendentals=rows * key_rows * heads,
        ),
        name="attend",
    )(*operands)


def stage_kernel(where, *refs):
    own = refs[0]
    pieces = refs[1:-2]
    out_ref, sem = refs[-2:]
    peers = out_ref.shape[0]
    rows = pieces[0].shape[0]
    here, core = where[0], where[1]
    copies = [pltpu.make_async_copy(own, out_ref.at[here], sem.at[0])]
    for index, piece in enumerate(pieces):
        source = lax.rem(here + peers - (1 + index // 2), peers)
        part = core if index % 2 == 0 else 1 - core
        copies.append(
            pltpu.make_async_copy(
                piece,
                out_ref.at[source, pl.ds(pl.multiple_of(part * rows, rows), rows)],
                sem.at[1 + index],
            )
        )
    for copy in copies:
        copy.start()
    for copy in copies:
        copy.wait()


def stage(where, own, pieces):
    peers = 1 + len(pieces) // 2
    hbm = pl.BlockSpec(memory_space=pltpu.HBM)
    return pl.pallas_call(
        stage_kernel,
        out_shape=pltpu.VMEM((peers,) + own.shape, own.dtype),
        in_specs=[pl.BlockSpec(memory_space=pltpu.SMEM)] + [hbm] * (1 + len(pieces)),
        out_specs=pl.BlockSpec(memory_space=pltpu.VMEM),
        scratch_shapes=[pltpu.SemaphoreType.DMA((1 + len(pieces),))],
        compiler_params=pltpu.CompilerParams(vmem_limit_bytes=24 * 1024 * 1024),
        cost_estimate=pl.CostEstimate(
            flops=2 * 10**8, bytes_accessed=4 * peers * own.size, transcendentals=0
        ),
        name="stage",
    )(where, own, *pieces)


GATE, SHIFT, SCALE, BIAS, NUMBERS = 0, 2, 4, 6, 7


def finish_kernel(
    w_ref,
    attn_hbm,
    hidden_hbm,
    table_hbm,
    w_final_hbm,
    small_hbm,
    out_ref,
    attn_ref,
    hidden_ref,
    table_ref,
    w_final_ref,
    small_ref,
    sem,
):
    pairs = (
        (attn_hbm, attn_ref),
        (hidden_hbm, hidden_ref),
        (table_hbm, table_ref),
        (w_final_hbm, w_final_ref),
        (small_hbm, small_ref),
    )
    copies = [pltpu.make_async_copy(a, b, sem.at[i]) for i, (a, b) in enumerate(pairs)]
    for copy in copies:
        copy.start()
    copies[0].wait()
    peers = w_ref.shape[0]
    rows = small_ref.shape[1]

    def of_both(at):
        return jnp.concatenate(
            [jnp.broadcast_to(table_ref[at + b : at + b + 1], (rows, D)) for b in range(2)], axis=0
        )

    projected = None
    for source in range(peers):
        left = jnp.concatenate([attn_ref[b, source] for b in range(2)], axis=0)
        term = jnp.dot(left, w_ref[source], preferred_element_type=jnp.float32)
        projected = term if projected is None else projected + term
    for copy in copies[1:]:
        copy.wait()
    mixed = hidden_ref[...].astype(jnp.float32) + of_both(GATE) * (
        projected + table_ref[BIAS : BIAS + 1]
    )
    normed = layer_norm(mixed)
    final_in = (normed * (1.0 + of_both(SCALE)) + of_both(SHIFT)).astype(jnp.bfloat16)
    velocity = (
        jnp.dot(final_in, w_final_ref[...], preferred_element_type=jnp.float32) + small_ref[2, 0:1]
    )

    def number(at):
        return table_ref[NUMBERS : NUMBERS + 1, at : at + 1]

    cond = velocity[:rows]
    uncond = velocity[rows:]
    guided = uncond + number(0) * (cond - uncond)
    latent = small_ref[0]
    denoised = latent - number(1) * guided
    blend = number(2) * denoised - number(3) * small_ref[1]
    out_ref[1] = denoised
    out_ref[0] = number(4) * latent - number(5) * blend


def finish(w_all, attn, hidden, table, w_final, small):
    _, rows, channels = small.shape
    depth = w_all.shape[0] * w_all.shape[1]
    hbm = pl.BlockSpec(memory_space=pltpu.HBM)
    vmem = pl.BlockSpec(memory_space=pltpu.VMEM)
    loaded = (attn, hidden, table, w_final, small)
    return pl.pallas_call(
        finish_kernel,
        out_shape=jax.ShapeDtypeStruct((2, rows, channels), jnp.float32),
        in_specs=[vmem] + [hbm] * len(loaded),
        out_specs=vmem,
        scratch_shapes=[pltpu.VMEM(x.shape, x.dtype) for x in loaded]
        + [pltpu.SemaphoreType.DMA((len(loaded),))],
        compiler_params=pltpu.CompilerParams(vmem_limit_bytes=32 * 1024 * 1024),
        cost_estimate=pl.CostEstimate(
            flops=4 * rows * depth * D, bytes_accessed=2 * depth * D, transcendentals=0
        ),
        name="finish",
    )(w_all, *loaded)


def body(
    img_hidden,
    txt_hidden,
    modulation,
    w_qkv,
    q_gain,
    k_gain,
    w_out,
    b_out,
    stale_kv,
    final_mod,
    w_final,
    b_final,
    latent,
    prev_denoised,
    guidance,
    step_index,
    step_count,
):
    head_width = w_out.shape[0]
    head_count = head_width // HD
    img_rows = img_hidden.shape[1]
    txt_rows = txt_hidden.shape[1]
    kv_rows = img_rows + txt_rows
    out_rows = latent.shape[0]
    patch_index = lax.axis_index("patch")
    cfg_index = lax.axis_index("cfg")
    head_index = lax.axis_index("head")
    head_total = lax.axis_size("head")

    patches = lax.axis_size("patch")
    reach = patches // 2
    ahead = [(i, (i + 1) % patches) for i in range(patches)]
    back = [(i, (i - 1) % patches) for i in range(patches)]
    swap = [(0, 1), (1, 0)]
    rising = falling = (stale_kv[0, 0], stale_kv[0, 1])
    arrived = []
    for step in range(1, reach):
        rising = tuple(lax.ppermute(x, "patch", ahead) for x in rising)
        falling = tuple(lax.ppermute(x, "patch", back) for x in falling)
        arrived.append((rising, falling))
    farthest = (lax.ppermute(rising[0], "patch", ahead), lax.ppermute(falling[1], "patch", back))

    half = w_out.shape[0] // 2
    w_half = lax.dynamic_slice_in_dim(w_out, cfg_index * half, half, 0)
    pieces = []
    for shift in range(1, head_total):
        mine = lax.ppermute(
            w_half, "head", [(i, (i + shift) % head_total) for i in range(head_total)]
        )
        pieces += [mine, lax.ppermute(mine, "cfg", swap)]
    hidden_rows = img_hidden.reshape(2, head_total, out_rows, D)
    hidden_mine = lax.dynamic_index_in_dim(hidden_rows, head_index, 1, keepdims=False)
    own_hidden = lax.dynamic_index_in_dim(hidden_mine, cfg_index, 0, keepdims=False)
    sent_hidden = lax.dynamic_index_in_dim(hidden_mine, 1 - cfg_index, 0, keepdims=False)
    other_hidden = lax.ppermute(sent_hidden, "cfg", swap)
    own_vecs = jnp.concatenate([modulation[0, 2:], final_mod[0]], axis=0)
    other_vecs = lax.ppermute(own_vecs, "cfg", swap)
    first = cfg_index == 0
    hidden = jnp.concatenate(
        [
            jnp.where(first, own_hidden, other_hidden),
            jnp.where(first, other_hidden, own_hidden),
        ],
        axis=0,
    )
    vecs = jnp.stack(
        [jnp.where(first, own_vecs, other_vecs), jnp.where(first, other_vecs, own_vecs)], axis=1
    )
    numbers = solver_scalars(guidance, step_index, step_count)
    table = jnp.concatenate(
        [vecs.reshape(6, D), b_out.reshape(1, D), jnp.pad(numbers, (0, D - 6)).reshape(1, D)]
    )
    small = jnp.stack([latent, prev_denoised, jnp.broadcast_to(b_final, latent.shape)])

    shift_vec = modulation[0, 0]
    scale_vec = modulation[0, 1]
    modded_img = (
        layer_norm(img_hidden[0].astype(jnp.float32)) * (1.0 + scale_vec) + shift_vec
    ).astype(jnp.bfloat16)
    modded_txt = (
        layer_norm(txt_hidden[0].astype(jnp.float32)) * (1.0 + scale_vec) + shift_vec
    ).astype(jnp.bfloat16)
    weight_flat = w_qkv.reshape(D, 3 * head_width)
    proj_img = jnp.dot(modded_img, weight_flat, preferred_element_type=jnp.float32).reshape(
        img_rows, 3, head_count, HD
    )
    proj_txt = jnp.dot(modded_txt, weight_flat, preferred_element_type=jnp.float32).reshape(
        txt_rows, 3, head_count, HD
    )
    positions = patch_index * img_rows + jnp.arange(img_rows, dtype=jnp.int32)
    queries = rotate(rms_norm(proj_img[:, 0], q_gain), positions, GRID_W).astype(jnp.bfloat16)
    img_keys = rotate(rms_norm(proj_img[:, 1], k_gain), positions, GRID_W).astype(jnp.bfloat16)
    img_vals = proj_img[:, 2].astype(jnp.bfloat16)
    txt_keys = rms_norm(proj_txt[:, 1], k_gain).astype(jnp.bfloat16)
    txt_vals = proj_txt[:, 2].astype(jnp.bfloat16)
    fresh_keys = jnp.concatenate([txt_keys, img_keys], axis=0)
    fresh_vals = jnp.concatenate([txt_vals, img_vals], axis=0)
    fresh_kv = jnp.stack(
        [fresh_keys.reshape(kv_rows, head_width), fresh_vals.reshape(kv_rows, head_width)]
    )

    queries = queries.reshape(img_rows, head_width)
    groups = [[(fresh_kv[0], fresh_kv[1])] + [b for pair in arrived[:2] for b in pair]]
    for at in range(2, reach - 2, 2):
        groups.append([b for pair in arrived[at : at + 2] for b in pair])
    done = 2 + 2 * (len(groups) - 1)
    groups += [[b for b in pair] for pair in arrived[done:]]
    state = None
    for group in groups:
        state = attend(queries, group, state, False)
    attn = attend(queries, [farthest], state, True)
    w_all = stage(jnp.stack([head_index, cfg_index]), w_out, pieces)
    shared = lax.all_to_all(
        attn.reshape(2 * head_total, out_rows, head_width), ("cfg", "head"), 0, 0, tiled=True
    ).reshape(2, head_total, out_rows, head_width)
    result = finish(w_all, shared, hidden, table, w_final, small)
    return (fresh_kv[None], result[0], result[1])


def solution(mesh):
    return jax.shard_map(
        body,
        mesh=mesh,
        in_specs=(
            P("cfg", ("groups", "patch"), None),
            P("cfg", ("groups", "patch"), None),
            P(("groups", "cfg"), None, None),
            P(None, None, "head"),
            P(),
            P(),
            P("head", None),
            P(),
            P("cfg", None, ("groups", "patch"), "head"),
            P(("groups", "cfg"), None, None),
            P(),
            P(),
            P(("groups", "patch", "cfg", "head"), None),
            P(("groups", "patch", "cfg", "head"), None),
            P("groups"),
            P(),
            P(),
        ),
        out_specs=(
            P("cfg", None, ("groups", "patch"), "head"),
            P(("groups", "patch", "cfg", "head"), None),
            P(("groups", "patch", "cfg", "head"), None),
        ),
        check_vma=False,
    )
```

```python
import functools
import math

import jax
import jax.numpy as jnp
from jax import lax
from jax.experimental import pallas as pl
from jax.experimental.pallas import tpu as pltpu
from jax.sharding import PartitionSpec as P

D = 3072
HD = 128
CH = 64
GRID_W = 128


epsilon = 1e-06
time_shift = 3.0


def layer_norm(values):
    mean_val = jnp.mean(values, axis=-1, keepdims=True)
    centered = values - mean_val
    variance = jnp.mean(centered * centered, axis=-1, keepdims=True)
    return centered * lax.rsqrt(variance + epsilon)


def turn_tables(patch_index, img_rows, txt_rows):
    quarter = HD // 4
    lane = jnp.arange(HD, dtype=jnp.int32)
    freqs = 10000.0 ** (-(lane % quarter).astype(jnp.float32) / quarter)
    row = jnp.arange(txt_rows + img_rows, dtype=jnp.int32) - txt_rows
    token = patch_index * img_rows + row
    place = jnp.where(lane[None] < HD // 2, (token // GRID_W)[:, None], (token % GRID_W)[:, None])
    angles = jnp.where(row[:, None] < 0, 0.0, place.astype(jnp.float32) * freqs[None])
    sign = jnp.where(lane % (HD // 2) < quarter, -1.0, 1.0)
    return jnp.stack([jnp.cos(angles), jnp.sin(angles) * sign[None]])


def noise_level(index, count):
    frac = 1.0 - index / count
    lift = math.exp(time_shift)
    return lift * frac / (lift * frac + 1.0 - frac)


def log_ratio(sigma_val):
    return jnp.log(1.0 - sigma_val) - jnp.log(sigma_val)


def solver_scalars(guidance, step_index, step_count):
    index = step_index[0].astype(jnp.float32)
    count = step_count[0].astype(jnp.float32)
    sigma_prev = noise_level(index - 1.0, count)
    sigma_now = noise_level(index, count)
    sigma_next = noise_level(index + 1.0, count)
    step_now = log_ratio(sigma_next) - log_ratio(sigma_now)
    step_prev = log_ratio(sigma_now) - log_ratio(sigma_prev)
    ratio = step_prev / step_now
    return jnp.stack(
        [
            guidance[0],
            sigma_now,
            1.0 + 0.5 / ratio,
            0.5 / ratio,
            sigma_next / sigma_now,
            (1.0 - sigma_next) * (jnp.exp(-step_now) - 1.0),
        ]
    )


def project_kernel(
    txt_ref, img_ref, mod_ref, wq_ref, wk_ref, wv_ref, gain_ref, turn_ref, q_ref, kv_ref, x_ref
):
    txt_rows = txt_ref.shape[0]
    width = wq_ref.shape[1]
    quarter = HD // 4
    at = 0
    for part in (txt_ref, img_ref):
        rows = part.shape[0]
        block = min(rows, 64)
        for start in range(0, rows, block):
            normed = layer_norm(part[start : start + block].astype(jnp.float32))
            x_ref[at : at + block] = (normed * (1.0 + mod_ref[1:2]) + mod_ref[0:1]).astype(
                jnp.bfloat16
            )
            at += block
    lane = lax.broadcasted_iota(jnp.int32, (1, HD), 1)
    early = lane % (HD // 2) < quarter

    def turned(values, gain):
        scaled = (
            values * lax.rsqrt(jnp.mean(values * values, axis=-1, keepdims=True) + epsilon) * gain
        )
        swapped = jnp.where(
            early, pltpu.roll(scaled, HD - quarter, 1), pltpu.roll(scaled, quarter, 1)
        )
        return (scaled * turn_ref[0] + swapped * turn_ref[1]).astype(jnp.bfloat16)

    for index, w_ref in enumerate((wk_ref, wv_ref, wq_ref)):
        proj = jnp.dot(x_ref[...], w_ref[...], preferred_element_type=jnp.float32)
        for head in range(width // HD):
            lanes = slice(head * HD, (head + 1) * HD)
            values = proj[:, lanes]
            if index == 0:
                kv_ref[0, :, lanes] = turned(values, gain_ref[1:2])
            elif index == 1:
                kv_ref[1, :, lanes] = values.astype(jnp.bfloat16)
            else:
                q_ref[:, lanes] = turned(values, gain_ref[0:1])[txt_rows:]


def project(txt, img, mod, wq, wk, wv, gains, turns):
    rows = txt.shape[0] + img.shape[0]
    width = wq.shape[1]
    operands = (txt, img, mod, wq, wk, wv, gains, turns)
    vmem = pl.BlockSpec(memory_space=pltpu.VMEM)
    return pl.pallas_call(
        project_kernel,
        out_shape=(
            jax.ShapeDtypeStruct((img.shape[0], width), jnp.bfloat16),
            jax.ShapeDtypeStruct((2, rows, width), jnp.bfloat16),
        ),
        in_specs=[vmem] * len(operands),
        out_specs=(vmem, vmem),
        scratch_shapes=[pltpu.VMEM((rows, D), jnp.bfloat16)],
        compiler_params=pltpu.CompilerParams(vmem_limit_bytes=32 * 1024 * 1024),
        cost_estimate=pl.CostEstimate(
            flops=6 * rows * D * width, bytes_accessed=6 * D * width, transcendentals=0
        ),
        name="project",
    )(*operands)


def attend_kernel(first, last, count, split, *refs):
    q_ref = refs[0]
    if split:
        pairs = [(refs[1], refs[2], 0)]
        refs = refs[3:]
    else:
        pairs = [(ref, ref, ref.shape[0] // 2) for ref in refs[1 : 1 + count]]
        refs = refs[1 + count :]
    key_rows = pairs[0][0].shape[0] - pairs[0][2]
    if not first:
        top_in, denom_in, acc_in = refs[:3]
        refs = refs[3:]
    heads = q_ref.shape[1] // HD
    scale = math.log2(math.e) * HD ** (-0.5)

    def attend_head(head, _):
        lanes = pl.ds(head * HD if last else pl.multiple_of(head * HD, HD), HD)
        query = q_ref[:, lanes]
        scores = [
            lax.dot_general(
                keys[:key_rows, lanes],
                query,
                (((1,), (1,)), ((), ())),
                preferred_element_type=jnp.float32,
            )
            for keys, _, _ in pairs
        ]
        top = functools.reduce(jnp.maximum, [jnp.max(s, axis=0, keepdims=True) for s in scores])
        if not first:
            top = jnp.maximum(top, top_in[head])
        shift = top * scale
        denom = None
        acc = None
        for score, (_, vals, offset) in zip(scores, pairs):
            expo = jnp.exp2(score * scale - shift)
            part = jnp.sum(expo, axis=0, keepdims=True)
            term = lax.dot_general(
                vals[offset : offset + key_rows, lanes],
                expo.astype(jnp.bfloat16),
                (((0,), (0,)), ((), ())),
                preferred_element_type=jnp.float32,
            )
            denom = part if denom is None else denom + part
            acc = term if acc is None else acc + term
        if not first:
            factor = jnp.exp2(top_in[head] * scale - shift)
            denom = denom + denom_in[head] * factor
            acc = acc + acc_in[head] * factor
        if last:
            refs[0][:, lanes] = (acc / denom).T.astype(jnp.bfloat16)
        else:
            refs[0][head] = top
            refs[1][head] = denom
            refs[2][head] = acc
        return 0

    if last:
        for head in range(heads):
            attend_head(head, 0)
    else:
        lax.fori_loop(0, heads, attend_head, 0)


def attend(queries, blocks, state, last):
    rows, width = queries.shape
    heads = width // HD
    key_rows = sum(block.shape[0] for block in blocks) // 2
    vmem = pl.BlockSpec(memory_space=pltpu.VMEM)
    row = jax.ShapeDtypeStruct((heads, 1, rows), jnp.float32)
    held = (row, row, jax.ShapeDtypeStruct((heads, HD, rows), jnp.float32))
    out_shape = jax.ShapeDtypeStruct((rows, width), jnp.bfloat16) if last else held
    first = state is None
    operands = [queries] + list(blocks) + ([] if first else list(state))
    return pl.pallas_call(
        functools.partial(attend_kernel, first, last, len(blocks), last),
        out_shape=out_shape,
        in_specs=[vmem] * len(operands),
        out_specs=vmem if last else (vmem,) * 3,
        compiler_params=pltpu.CompilerParams(vmem_limit_bytes=24 * 1024 * 1024),
        cost_estimate=pl.CostEstimate(
            flops=4 * rows * key_rows * width,
            bytes_accessed=4 * key_rows * width,
            transcendentals=rows * key_rows * heads,
        ),
        name="attend",
    )(*operands)


def stage_kernel(where, *refs):
    own = refs[0]
    pieces = refs[1:-2]
    out_ref, sem = refs[-2:]
    peers = out_ref.shape[0]
    rows = pieces[0].shape[0]
    here, core = where[0], where[1]
    copies = [pltpu.make_async_copy(own, out_ref.at[here], sem.at[0])]
    for index, piece in enumerate(pieces):
        source = lax.rem(here + peers - (1 + index // 2), peers)
        part = core if index % 2 == 0 else 1 - core
        copies.append(
            pltpu.make_async_copy(
                piece,
                out_ref.at[source, pl.ds(pl.multiple_of(part * rows, rows), rows)],
                sem.at[1 + index],
            )
        )
    for copy in copies:
        copy.start()
    for copy in copies:
        copy.wait()


def stage(where, own, pieces):
    peers = 1 + len(pieces) // 2
    hbm = pl.BlockSpec(memory_space=pltpu.HBM)
    return pl.pallas_call(
        stage_kernel,
        out_shape=pltpu.VMEM((peers,) + own.shape, own.dtype),
        in_specs=[pl.BlockSpec(memory_space=pltpu.SMEM)] + [hbm] * (1 + len(pieces)),
        out_specs=pl.BlockSpec(memory_space=pltpu.VMEM),
        scratch_shapes=[pltpu.SemaphoreType.DMA((1 + len(pieces),))],
        compiler_params=pltpu.CompilerParams(vmem_limit_bytes=24 * 1024 * 1024),
        cost_estimate=pl.CostEstimate(
            flops=2 * 10**8, bytes_accessed=4 * peers * own.size, transcendentals=0
        ),
        name="stage",
    )(where, own, *pieces)


GATE, SHIFT, SCALE, BIAS, NUMBERS = 0, 2, 4, 6, 7


def finish_kernel(
    w_ref,
    attn_hbm,
    hidden_hbm,
    table_hbm,
    w_final_hbm,
    small_hbm,
    out_ref,
    attn_ref,
    hidden_ref,
    table_ref,
    w_final_ref,
    small_ref,
    sem,
):
    pairs = (
        (attn_hbm, attn_ref),
        (hidden_hbm, hidden_ref),
        (table_hbm, table_ref),
        (w_final_hbm, w_final_ref),
        (small_hbm, small_ref),
    )
    copies = [pltpu.make_async_copy(a, b, sem.at[i]) for i, (a, b) in enumerate(pairs)]
    for copy in copies:
        copy.start()
    copies[0].wait()
    peers = w_ref.shape[0]
    rows = small_ref.shape[1]

    def of_both(at):
        return jnp.concatenate(
            [jnp.broadcast_to(table_ref[at + b : at + b + 1], (rows, D)) for b in range(2)], axis=0
        )

    projected = None
    for source in range(peers):
        left = jnp.concatenate([attn_ref[b, source] for b in range(2)], axis=0)
        term = jnp.dot(left, w_ref[source], preferred_element_type=jnp.float32)
        projected = term if projected is None else projected + term
    for copy in copies[1:]:
        copy.wait()
    mixed = hidden_ref[...].astype(jnp.float32) + of_both(GATE) * (
        projected + table_ref[BIAS : BIAS + 1]
    )
    normed = layer_norm(mixed)
    final_in = (normed * (1.0 + of_both(SCALE)) + of_both(SHIFT)).astype(jnp.bfloat16)
    velocity = (
        jnp.dot(final_in, w_final_ref[...], preferred_element_type=jnp.float32) + small_ref[2, 0:1]
    )

    def number(at):
        return table_ref[NUMBERS : NUMBERS + 1, at : at + 1]

    cond = velocity[:rows]
    uncond = velocity[rows:]
    guided = uncond + number(0) * (cond - uncond)
    latent = small_ref[0]
    denoised = latent - number(1) * guided
    blend = number(2) * denoised - number(3) * small_ref[1]
    out_ref[1] = denoised
    out_ref[0] = number(4) * latent - number(5) * blend


def finish(w_all, attn, hidden, table, w_final, small):
    _, rows, channels = small.shape
    depth = w_all.shape[0] * w_all.shape[1]
    hbm = pl.BlockSpec(memory_space=pltpu.HBM)
    vmem = pl.BlockSpec(memory_space=pltpu.VMEM)
    loaded = (attn, hidden, table, w_final, small)
    return pl.pallas_call(
        finish_kernel,
        out_shape=jax.ShapeDtypeStruct((2, rows, channels), jnp.float32),
        in_specs=[vmem] + [hbm] * len(loaded),
        out_specs=vmem,
        scratch_shapes=[pltpu.VMEM(x.shape, x.dtype) for x in loaded]
        + [pltpu.SemaphoreType.DMA((len(loaded),))],
        compiler_params=pltpu.CompilerParams(vmem_limit_bytes=32 * 1024 * 1024),
        cost_estimate=pl.CostEstimate(
            flops=4 * rows * depth * D, bytes_accessed=2 * depth * D, transcendentals=0
        ),
        name="finish",
    )(w_all, *loaded)


def body(
    img_hidden,
    txt_hidden,
    modulation,
    w_qkv,
    q_gain,
    k_gain,
    w_out,
    b_out,
    stale_kv,
    final_mod,
    w_final,
    b_final,
    latent,
    prev_denoised,
    guidance,
    step_index,
    step_count,
):
    head_width = w_out.shape[0]
    img_rows = img_hidden.shape[1]
    txt_rows = txt_hidden.shape[1]
    kv_rows = img_rows + txt_rows
    out_rows = latent.shape[0]
    patch_index = lax.axis_index("patch")
    cfg_index = lax.axis_index("cfg")
    head_index = lax.axis_index("head")
    head_total = lax.axis_size("head")

    patches = lax.axis_size("patch")
    reach = patches // 2
    ahead = [(i, (i + 1) % patches) for i in range(patches)]
    back = [(i, (i - 1) % patches) for i in range(patches)]
    swap = [(0, 1), (1, 0)]
    half = w_out.shape[0] // 2
    w_half = lax.dynamic_slice_in_dim(w_out, cfg_index * half, half, 0)
    pieces = []
    for shift in range(1, head_total):
        mine = lax.ppermute(
            w_half, "head", [(i, (i + shift) % head_total) for i in range(head_total)]
        )
        pieces += [mine, lax.ppermute(mine, "cfg", swap)]
    hidden_rows = img_hidden.reshape(2, head_total, out_rows, D)
    hidden_mine = lax.dynamic_index_in_dim(hidden_rows, head_index, 1, keepdims=False)
    own_hidden = lax.dynamic_index_in_dim(hidden_mine, cfg_index, 0, keepdims=False)
    sent_hidden = lax.dynamic_index_in_dim(hidden_mine, 1 - cfg_index, 0, keepdims=False)
    other_hidden = lax.ppermute(sent_hidden, "cfg", swap)
    own_vecs = jnp.concatenate([modulation[0, 2:], final_mod[0]], axis=0)
    other_vecs = lax.ppermute(own_vecs, "cfg", swap)
    first = cfg_index == 0
    hidden = jnp.concatenate(
        [
            jnp.where(first, own_hidden, other_hidden),
            jnp.where(first, other_hidden, own_hidden),
        ],
        axis=0,
    )
    vecs = jnp.stack(
        [jnp.where(first, own_vecs, other_vecs), jnp.where(first, other_vecs, own_vecs)], axis=1
    )
    numbers = solver_scalars(guidance, step_index, step_count)
    table = jnp.concatenate(
        [vecs.reshape(6, D), b_out.reshape(1, D), jnp.pad(numbers, (0, D - 6)).reshape(1, D)]
    )
    small = jnp.stack([latent, prev_denoised, jnp.broadcast_to(b_final, latent.shape)])

    gains = jnp.stack([q_gain, k_gain])
    stale = stale_kv.reshape(2 * kv_rows, head_width)
    rising = falling = stale
    arrived = []
    held = {}

    def work(step):
        if step == 1:
            held["wk"], held["wv"] = w_qkv[:, 1], w_qkv[:, 2]
            return held["wk"], held["wv"]
        if step == 2:
            held["wq"] = w_qkv[:, 0]
            held["turns"] = turn_tables(patch_index, img_rows, txt_rows)
            return held["wq"], held["turns"]
        if step == 3:
            held["q"], held["fresh"] = project(
                txt_hidden[0],
                img_hidden[0],
                modulation[0, :2],
                held["wq"],
                held["wk"],
                held["wv"],
                gains,
                held["turns"],
            )
            return held["q"], held["fresh"]
        if step == 4:
            group = [held["fresh"].reshape(stale.shape)] + [x for p in arrived[:2] for x in p]
        elif step == 5:
            group = [x for p in arrived[2:4] for x in p]
        else:
            group = list(arrived[step - 2])
        held["state"] = attend(held["q"], group, held.get("state"), False)
        return held["state"]

    for step in range(1, reach + 1):
        if step < reach:
            going = (rising, falling)
        else:
            going = (rising[:kv_rows], falling[kv_rows:])
        going = (lax.ppermute(going[0], "patch", ahead), lax.ppermute(going[1], "patch", back))
        made = work(step)
        arrived.append(going)
        if step < reach:
            rising, falling, *tied = lax.optimization_barrier((*going, *made))
            if step == 1:
                held["wk"], held["wv"] = tied
            elif step == 2:
                held["wq"], held["turns"] = tied
            elif step == 3:
                held["q"], held["fresh"] = tied
            else:
                held["state"] = tuple(tied)
    fresh_kv = held["fresh"]
    attn = attend(held["q"], arrived[-1], held["state"], True)
    w_all = stage(jnp.stack([head_index, cfg_index]), w_out, pieces)
    shared = lax.all_to_all(
        attn.reshape(2 * head_total, out_rows, head_width), ("cfg", "head"), 0, 0, tiled=True
    ).reshape(2, head_total, out_rows, head_width)
    w_all = pltpu.with_memory_space_constraint(w_all, pltpu.VMEM)
    result = finish(w_all, shared, hidden, table, w_final, small)
    return (fresh_kv[None], result[0], result[1])


def solution(mesh):
    return jax.shard_map(
        body,
        mesh=mesh,
        in_specs=(
            P("cfg", ("groups", "patch"), None),
            P("cfg", ("groups", "patch"), None),
            P(("groups", "cfg"), None, None),
            P(None, None, "head"),
            P(),
            P(),
            P("head", None),
            P(),
            P("cfg", None, ("groups", "patch"), "head"),
            P(("groups", "cfg"), None, None),
            P(),
            P(),
            P(("groups", "patch", "cfg", "head"), None),
            P(("groups", "patch", "cfg", "head"), None),
            P("groups"),
            P(),
            P(),
        ),
        out_specs=(
            P("cfg", None, ("groups", "patch"), "head"),
            P(("groups", "patch", "cfg", "head"), None),
            P(("groups", "patch", "cfg", "head"), None),
        ),
        check_vma=False,
    )
```

```python
import functools
import math

import jax
import jax.numpy as jnp
from jax import lax
from jax.experimental import pallas as pl
from jax.experimental.pallas import tpu as pltpu
from jax.sharding import PartitionSpec as P

D = 3072
HD = 128
CH = 64
GRID_W = 128


epsilon = 1e-06
time_shift = 3.0


def layer_norm(values):
    mean_val = jnp.mean(values, axis=-1, keepdims=True)
    centered = values - mean_val
    variance = jnp.mean(centered * centered, axis=-1, keepdims=True)
    return centered * lax.rsqrt(variance + epsilon)


def turn_tables(patch_index, img_rows, txt_rows):
    quarter = HD // 4
    lane = jnp.arange(HD, dtype=jnp.int32)
    freqs = 10000.0 ** (-(lane % quarter).astype(jnp.float32) / quarter)
    row = jnp.arange(txt_rows + img_rows, dtype=jnp.int32) - txt_rows
    token = patch_index * img_rows + row
    place = jnp.where(lane[None] < HD // 2, (token // GRID_W)[:, None], (token % GRID_W)[:, None])
    angles = jnp.where(row[:, None] < 0, 0.0, place.astype(jnp.float32) * freqs[None])
    sign = jnp.where(lane % (HD // 2) < quarter, -1.0, 1.0)
    return jnp.stack([jnp.cos(angles), jnp.sin(angles) * sign[None]])


def noise_level(index, count):
    frac = 1.0 - index / count
    lift = math.exp(time_shift)
    return lift * frac / (lift * frac + 1.0 - frac)


def log_ratio(sigma_val):
    return jnp.log(1.0 - sigma_val) - jnp.log(sigma_val)


def project_kernel(
    txt_ref, img_ref, mod_ref, wq_ref, wk_ref, wv_ref, gain_ref, turn_ref, q_ref, kv_ref, x_ref
):
    txt_rows = txt_ref.shape[0]
    width = wq_ref.shape[1]
    quarter = HD // 4
    at = 0
    for part in (txt_ref, img_ref):
        rows = part.shape[0]
        block = min(rows, 64)
        for start in range(0, rows, block):
            normed = layer_norm(part[start : start + block].astype(jnp.float32))
            x_ref[at : at + block] = (normed * (1.0 + mod_ref[1:2]) + mod_ref[0:1]).astype(
                jnp.bfloat16
            )
            at += block
    lane = lax.broadcasted_iota(jnp.int32, (1, HD), 1)
    early = lane % (HD // 2) < quarter

    def turned(values, gain):
        scaled = (
            values * lax.rsqrt(jnp.mean(values * values, axis=-1, keepdims=True) + epsilon) * gain
        )
        swapped = jnp.where(
            early, pltpu.roll(scaled, HD - quarter, 1), pltpu.roll(scaled, quarter, 1)
        )
        return (scaled * turn_ref[0] + swapped * turn_ref[1]).astype(jnp.bfloat16)

    for index, w_ref in enumerate((wk_ref, wv_ref, wq_ref)):
        proj = jnp.dot(x_ref[...], w_ref[...], preferred_element_type=jnp.float32)
        for head in range(width // HD):
            lanes = slice(head * HD, (head + 1) * HD)
            values = proj[:, lanes]
            if index == 0:
                kv_ref[0, :, lanes] = turned(values, gain_ref[1:2])
            elif index == 1:
                kv_ref[1, :, lanes] = values.astype(jnp.bfloat16)
            else:
                q_ref[:, lanes] = turned(values, gain_ref[0:1])[txt_rows:]


def project(txt, img, mod, wq, wk, wv, gains, turns):
    rows = txt.shape[0] + img.shape[0]
    width = wq.shape[1]
    operands = (txt, img, mod, wq, wk, wv, gains, turns)
    vmem = pl.BlockSpec(memory_space=pltpu.VMEM)
    return pl.pallas_call(
        project_kernel,
        out_shape=(
            jax.ShapeDtypeStruct((img.shape[0], width), jnp.bfloat16),
            jax.ShapeDtypeStruct((2, rows, width), jnp.bfloat16),
        ),
        in_specs=[vmem] * len(operands),
        out_specs=(vmem, vmem),
        scratch_shapes=[pltpu.VMEM((rows, D), jnp.bfloat16)],
        compiler_params=pltpu.CompilerParams(vmem_limit_bytes=14 * 1024 * 1024),
        cost_estimate=pl.CostEstimate(
            flops=6 * rows * D * width, bytes_accessed=6 * D * width, transcendentals=0
        ),
        name="project",
    )(*operands)


def attend_kernel(first, last, count, split, *refs):
    q_ref = refs[0]
    if split:
        pairs = [(refs[1], refs[2], 0)]
        refs = refs[3:]
    else:
        pairs = [(ref, ref, ref.shape[0] // 2) for ref in refs[1 : 1 + count]]
        refs = refs[1 + count :]
    key_rows = pairs[0][0].shape[0] - pairs[0][2]
    if not first:
        top_in, denom_in, acc_in = refs[:3]
        refs = refs[3:]
    heads = q_ref.shape[1] // HD
    scale = math.log2(math.e) * HD ** (-0.5)

    def attend_head(head, _):
        lanes = pl.ds(head * HD if last else pl.multiple_of(head * HD, HD), HD)
        query = q_ref[:, lanes]
        scores = [
            lax.dot_general(
                keys[:key_rows, lanes],
                query,
                (((1,), (1,)), ((), ())),
                preferred_element_type=jnp.float32,
            )
            for keys, _, _ in pairs
        ]
        top = functools.reduce(jnp.maximum, [jnp.max(s, axis=0, keepdims=True) for s in scores])
        if not first:
            top = jnp.maximum(top, top_in[head])
        shift = top * scale
        denom = None
        acc = None
        for score, (_, vals, offset) in zip(scores, pairs):
            expo = jnp.exp2(score * scale - shift)
            part = jnp.sum(expo, axis=0, keepdims=True)
            term = lax.dot_general(
                vals[offset : offset + key_rows, lanes],
                expo.astype(jnp.bfloat16),
                (((0,), (0,)), ((), ())),
                preferred_element_type=jnp.float32,
            )
            denom = part if denom is None else denom + part
            acc = term if acc is None else acc + term
        if not first:
            factor = jnp.exp2(top_in[head] * scale - shift)
            denom = denom + denom_in[head] * factor
            acc = acc + acc_in[head] * factor
        if last:
            refs[0][:, lanes] = (acc / denom).T.astype(jnp.bfloat16)
        else:
            refs[0][head] = top
            refs[1][head] = denom
            refs[2][head] = acc
        return 0

    if last:
        for head in range(heads):
            attend_head(head, 0)
    else:
        lax.fori_loop(0, heads, attend_head, 0)


def attend(queries, blocks, state, last):
    rows, width = queries.shape
    heads = width // HD
    key_rows = sum(block.shape[0] for block in blocks) // 2
    vmem = pl.BlockSpec(memory_space=pltpu.VMEM)
    row = jax.ShapeDtypeStruct((heads, 1, rows), jnp.float32)
    held = (row, row, jax.ShapeDtypeStruct((heads, HD, rows), jnp.float32))
    out_shape = jax.ShapeDtypeStruct((rows, width), jnp.bfloat16) if last else held
    first = state is None
    operands = [queries] + list(blocks) + ([] if first else list(state))
    return pl.pallas_call(
        functools.partial(attend_kernel, first, last, len(blocks), last),
        out_shape=out_shape,
        in_specs=[vmem] * len(operands),
        out_specs=vmem if last else (vmem,) * 3,
        compiler_params=pltpu.CompilerParams(vmem_limit_bytes=8 * 1024 * 1024),
        cost_estimate=pl.CostEstimate(
            flops=4 * rows * key_rows * width,
            bytes_accessed=4 * key_rows * width,
            transcendentals=rows * key_rows * heads,
        ),
        name="attend",
    )(*operands)


def finish_kernel(where, guidance, step_index, step_count, *refs):
    (
        attn_hbm,
        own_hidden,
        other_hidden,
        own_vecs,
        other_vecs,
        b_out,
        w_final,
        b_final,
        latent,
        prev,
        own_w,
    ) = refs[:11]
    (
        next_out,
        denoised_out,
        w_ref,
        attn_ref,
        hidden_ref,
        vecs_ref,
        b_out_ref,
        w_final_ref,
        b_final_ref,
        latent_ref,
        prev_ref,
        sem,
    ) = refs[-12:]
    pieces = refs[11:-12]
    peers = w_ref.shape[0]
    half = pieces[0].shape[0]
    here, core = where[0], where[1]
    rows, channels = latent_ref.shape
    order = [here]
    groups = [[(attn_hbm, attn_ref)], [(own_w, w_ref.at[here])]]
    for shift in range(1, peers):
        source = lax.rem(here + peers - shift, peers)
        group = []
        for index in range(2):
            part = core if index == 0 else 1 - core
            span = pl.ds(pl.multiple_of(part * half, half), half)
            group.append((pieces[2 * shift - 2 + index], w_ref.at[source, span]))
        order.append(source)
        groups.append(group)
    groups.append(
        [
            (own_hidden, hidden_ref.at[core]),
            (other_hidden, hidden_ref.at[1 - core]),
            (own_vecs, vecs_ref.at[core]),
            (other_vecs, vecs_ref.at[1 - core]),
            (b_out, b_out_ref),
            (w_final, w_final_ref),
            (b_final, b_final_ref),
            (latent, latent_ref),
            (prev, prev_ref),
        ]
    )
    copies = []
    at = 0
    for group in groups:
        copies.append([pltpu.make_async_copy(*p, sem.at[at + i]) for i, p in enumerate(group)])
        at += len(group)
    for group in copies:
        for copy in group:
            copy.start()

    def arrived(at):
        for copy in copies[at]:
            copy.wait()

    def of_both(at):
        return jnp.concatenate(
            [jnp.broadcast_to(vecs_ref[b, at : at + 1], (rows, D)) for b in range(2)], axis=0
        )

    index = jnp.full((1, channels), step_index[0], jnp.int32).astype(jnp.float32)
    count = jnp.full((1, channels), step_count[0], jnp.int32).astype(jnp.float32)
    sigma_prev = noise_level(index - 1.0, count)
    sigma_now = noise_level(index, count)
    sigma_next = noise_level(index + 1.0, count)
    step_now = log_ratio(sigma_next) - log_ratio(sigma_now)
    step_prev = log_ratio(sigma_now) - log_ratio(sigma_prev)
    ratio = step_prev / step_now
    fade = (1.0 - sigma_next) * (jnp.exp(-step_now) - 1.0)

    arrived(0)
    projected = None
    for step, source in enumerate(order):
        arrived(1 + step)
        left = jnp.concatenate([attn_ref[b, source] for b in range(2)], axis=0)
        term = jnp.dot(left, w_ref[source], preferred_element_type=jnp.float32)
        projected = term if projected is None else projected + term
    arrived(-1)
    hidden = hidden_ref[...].reshape(2 * rows, D).astype(jnp.float32)
    mixed = hidden + of_both(0) * (projected + b_out_ref[...])
    normed = layer_norm(mixed)
    final_in = (normed * (1.0 + of_both(2)) + of_both(1)).astype(jnp.bfloat16)
    velocity = (
        lax.dot_general(
            final_in, w_final_ref[...], (((1,), (1,)), ((), ())), preferred_element_type=jnp.float32
        )
        + b_final_ref[...]
    )
    cond = velocity[:rows]
    uncond = velocity[rows:]
    guided = uncond + guidance[0] * (cond - uncond)
    denoised = latent_ref[...] - sigma_now * guided
    blend = (1.0 + 0.5 / ratio) * denoised - 0.5 / ratio * prev_ref[...]
    denoised_out[...] = denoised
    next_out[...] = sigma_next / sigma_now * latent_ref[...] - fade * blend


def finish(scalars, loaded, own_w, pieces):
    attn, hidden, _, vecs, _, b_out, w_final, b_final, latent, prev = loaded
    rows, channels = latent.shape
    peers = 1 + len(pieces) // 2
    depth = peers * own_w.shape[0]
    copies = len(loaded) + 1 + len(pieces)
    hbm = pl.BlockSpec(memory_space=pltpu.HBM)
    vmem = pl.BlockSpec(memory_space=pltpu.VMEM)
    smem = pl.BlockSpec(memory_space=pltpu.SMEM)
    out = jax.ShapeDtypeStruct(latent.shape, jnp.float32)
    return pl.pallas_call(
        finish_kernel,
        out_shape=(out, out),
        in_specs=[smem] * len(scalars) + [hbm] * copies,
        out_specs=(vmem, vmem),
        scratch_shapes=[
            pltpu.VMEM((peers,) + own_w.shape, own_w.dtype),
            pltpu.VMEM(attn.shape, attn.dtype),
            pltpu.VMEM((2,) + hidden.shape, hidden.dtype),
            pltpu.VMEM((2,) + vecs.shape, vecs.dtype),
        ]
        + [pltpu.VMEM(x.shape, x.dtype) for x in (b_out, w_final, b_final, latent, prev)]
        + [pltpu.SemaphoreType.DMA((copies,))],
        compiler_params=pltpu.CompilerParams(vmem_limit_bytes=20 * 1024 * 1024),
        cost_estimate=pl.CostEstimate(
            flops=4 * rows * depth * D, bytes_accessed=2 * depth * D, transcendentals=0
        ),
        name="finish",
    )(*scalars, *loaded, own_w, *pieces)


def body(
    img_hidden,
    txt_hidden,
    modulation,
    w_qkv,
    q_gain,
    k_gain,
    w_out,
    b_out,
    stale_kv,
    final_mod,
    w_final,
    b_final,
    latent,
    prev_denoised,
    guidance,
    step_index,
    step_count,
):
    head_width = w_out.shape[0]
    img_rows = img_hidden.shape[1]
    txt_rows = txt_hidden.shape[1]
    kv_rows = img_rows + txt_rows
    out_rows = latent.shape[0]
    patch_index = lax.axis_index("patch")
    cfg_index = lax.axis_index("cfg")
    head_index = lax.axis_index("head")
    head_total = lax.axis_size("head")

    patches = lax.axis_size("patch")
    reach = patches // 2
    ahead = [(i, (i + 1) % patches) for i in range(patches)]
    back = [(i, (i - 1) % patches) for i in range(patches)]
    swap = [(0, 1), (1, 0)]
    hidden_rows = img_hidden.reshape(2, head_total, out_rows, D)
    hidden_mine = lax.dynamic_index_in_dim(hidden_rows, head_index, 1, keepdims=False)
    own_hidden = lax.dynamic_index_in_dim(hidden_mine, cfg_index, 0, keepdims=False)
    sent_hidden = lax.dynamic_index_in_dim(hidden_mine, 1 - cfg_index, 0, keepdims=False)
    own_vecs = jnp.concatenate([modulation[0, 2:], final_mod[0]], axis=0)
    gains = jnp.stack([q_gain, k_gain])
    stale = stale_kv.reshape(2 * kv_rows, head_width)
    rising = falling = stale
    arrived = []
    held = {}

    def work(step):
        if step == 1:
            held["wk"], held["wv"] = w_qkv[:, 1], w_qkv[:, 2]
            return held["wk"], held["wv"]
        if step == 2:
            held["wq"] = w_qkv[:, 0]
            held["turns"] = turn_tables(patch_index, img_rows, txt_rows)
            return held["wq"], held["turns"]
        if step == 3:
            held["q"], held["fresh"] = project(
                txt_hidden[0],
                img_hidden[0],
                modulation[0, :2],
                held["wq"],
                held["wk"],
                held["wv"],
                gains,
                held["turns"],
            )
            return held["q"], held["fresh"]
        if step == 4:
            group = [held["fresh"].reshape(stale.shape)] + [x for p in arrived[:2] for x in p]
        elif step == 5:
            group = [x for p in arrived[2:4] for x in p]
        else:
            group = list(arrived[step - 2])
        held["state"] = attend(held["q"], group, held.get("state"), False)
        return held["state"]

    for step in range(1, reach + 1):
        if step < reach:
            going = (rising, falling)
        else:
            going = (rising[:kv_rows], falling[kv_rows:])
        going = (lax.ppermute(going[0], "patch", ahead), lax.ppermute(going[1], "patch", back))
        made = work(step)
        arrived.append(going)
        if step < reach:
            if step == reach - 2:
                other_hidden = lax.ppermute(sent_hidden, "cfg", swap)
                other_vecs = lax.ppermute(own_vecs, "cfg", swap)
                made = (*made, other_hidden, other_vecs)
            rising, falling, *tied = lax.optimization_barrier((*going, *made))
            if step == reach - 2:
                *tied, other_hidden, other_vecs = tied
            if step == 3:
                (w_tied,) = lax.optimization_barrier((w_out, rising))[:1]
                half = w_out.shape[0] // 2
                w_half = lax.dynamic_slice_in_dim(w_tied, cfg_index * half, half, 0)
                pieces = []
                for shift in range(1, head_total):
                    ring = [(i, (i + shift) % head_total) for i in range(head_total)]
                    mine = lax.ppermute(w_half, "head", ring)
                    pieces += [mine, lax.ppermute(mine, "cfg", swap)]
            if step == 1:
                held["wk"], held["wv"] = tied
            elif step == 2:
                held["wq"], held["turns"] = tied
            elif step == 3:
                held["q"], held["fresh"] = tied
            else:
                held["state"] = tuple(tied)
    fresh_kv = held["fresh"]
    attn = attend(held["q"], arrived[-1], held["state"], True)
    shared = lax.all_to_all(
        attn.reshape(2 * head_total, out_rows, head_width), ("cfg", "head"), 0, 0, tiled=True
    ).reshape(2, head_total, out_rows, head_width)
    where = jnp.stack([head_index, cfg_index])
    loaded = (
        shared,
        own_hidden,
        other_hidden,
        own_vecs,
        other_vecs,
        b_out.reshape(1, D),
        w_final.T,
        b_final.reshape(1, CH),
        latent,
        prev_denoised,
    )
    next_latent, denoised = finish(
        (where, guidance, step_index, step_count), loaded, w_out, pieces
    )
    return (fresh_kv[None], next_latent, denoised)


def solution(mesh):
    return jax.shard_map(
        body,
        mesh=mesh,
        in_specs=(
            P("cfg", ("groups", "patch"), None),
            P("cfg", ("groups", "patch"), None),
            P(("groups", "cfg"), None, None),
            P(None, None, "head"),
            P(),
            P(),
            P("head", None),
            P(),
            P("cfg", None, ("groups", "patch"), "head"),
            P(("groups", "cfg"), None, None),
            P(),
            P(),
            P(("groups", "patch", "cfg", "head"), None),
            P(("groups", "patch", "cfg", "head"), None),
            P("groups"),
            P(),
            P(),
        ),
        out_specs=(
            P("cfg", None, ("groups", "patch"), "head"),
            P(("groups", "patch", "cfg", "head"), None),
            P(("groups", "patch", "cfg", "head"), None),
        ),
        check_vma=False,
    )
```

```python
import functools
import math

import jax
import jax.numpy as jnp
from jax import lax
from jax.experimental import pallas as pl
from jax.experimental.pallas import tpu as pltpu
from jax.sharding import PartitionSpec as P


D = 3072
HD = 128
CH = 64
GRID_W = 128


epsilon = 1e-06
time_shift = 3.0


def layer_norm(values):
    mean_val = jnp.mean(values, axis=-1, keepdims=True)
    centered = values - mean_val
    variance = jnp.mean(centered * centered, axis=-1, keepdims=True)
    return centered * lax.rsqrt(variance + epsilon)


def turn_tables(patch_index, img_rows, txt_rows):
    quarter = HD // 4
    lane = jnp.arange(HD, dtype=jnp.int32)
    freqs = 10000.0 ** (-(lane % quarter).astype(jnp.float32) / quarter)
    row = jnp.arange(txt_rows + img_rows, dtype=jnp.int32) - txt_rows
    token = patch_index * img_rows + row
    place = jnp.where(lane[None] < HD // 2, (token // GRID_W)[:, None], (token % GRID_W)[:, None])
    angles = jnp.where(row[:, None] < 0, 0.0, place.astype(jnp.float32) * freqs[None])
    sign = jnp.where(lane % (HD // 2) < quarter, -1.0, 1.0)
    return jnp.stack([jnp.cos(angles), jnp.sin(angles) * sign[None]])


def noise_level(index, count):
    frac = 1.0 - index / count
    lift = math.exp(time_shift)
    return lift * frac / (lift * frac + 1.0 - frac)


def log_ratio(sigma_val):
    return jnp.log(1.0 - sigma_val) - jnp.log(sigma_val)


def project_kernel(
    txt_ref,
    img_ref,
    mod_ref,
    wq_hbm,
    wk_hbm,
    wv_hbm,
    gain_ref,
    turn_ref,
    q_ref,
    kv_ref,
    x_ref,
    w_ref,
    sem,
):
    txt_rows = txt_ref.shape[0]
    width = w_ref.shape[2]
    quarter = HD // 4
    copies = [
        pltpu.make_async_copy(w_hbm, w_ref.at[i], sem.at[i])
        for i, w_hbm in enumerate((wk_hbm, wv_hbm, wq_hbm))
    ]
    for copy in copies:
        copy.start()
    at = 0
    for part in (txt_ref, img_ref):
        rows = part.shape[0]
        block = min(rows, 64)
        for start in range(0, rows, block):
            normed = layer_norm(part[start : start + block].astype(jnp.float32))
            x_ref[at : at + block] = (normed * (1.0 + mod_ref[1:2]) + mod_ref[0:1]).astype(
                jnp.bfloat16
            )
            at += block
    lane = lax.broadcasted_iota(jnp.int32, (1, HD), 1)
    early = lane % (HD // 2) < quarter

    def turned(values, gain):
        scaled = (
            values * lax.rsqrt(jnp.mean(values * values, axis=-1, keepdims=True) + epsilon) * gain
        )
        swapped = jnp.where(
            early, pltpu.roll(scaled, HD - quarter, 1), pltpu.roll(scaled, quarter, 1)
        )
        return (scaled * turn_ref[0] + swapped * turn_ref[1]).astype(jnp.bfloat16)

    for index, copy in enumerate(copies):
        copy.wait()
        proj = jnp.dot(x_ref[...], w_ref[index], preferred_element_type=jnp.float32)
        for head in range(width // HD):
            lanes = slice(head * HD, (head + 1) * HD)
            values = proj[:, lanes]
            if index == 0:
                kv_ref[0, :, lanes] = turned(values, gain_ref[1:2])
            elif index == 1:
                kv_ref[1, :, lanes] = values.astype(jnp.bfloat16)
            else:
                q_ref[:, lanes] = turned(values, gain_ref[0:1])[txt_rows:]


def project(txt, img, mod, wq, wk, wv, gains, turns):
    rows = txt.shape[0] + img.shape[0]
    width = wq.shape[1]
    wq, wk, wv = (pltpu.with_memory_space_constraint(w, pltpu.HBM) for w in (wq, wk, wv))
    operands = (txt, img, mod, wq, wk, wv, gains, turns)
    vmem = pl.BlockSpec(memory_space=pltpu.VMEM)
    hbm = pl.BlockSpec(memory_space=pltpu.HBM)
    return pl.pallas_call(
        project_kernel,
        out_shape=(
            jax.ShapeDtypeStruct((img.shape[0], width), jnp.bfloat16),
            jax.ShapeDtypeStruct((2, rows, width), jnp.bfloat16),
        ),
        in_specs=[vmem] * 3 + [hbm] * 3 + [vmem] * 2,
        out_specs=(vmem, vmem),
        scratch_shapes=[
            pltpu.VMEM((rows, D), jnp.bfloat16),
            pltpu.VMEM((3,) + wq.shape, jnp.bfloat16),
            pltpu.SemaphoreType.DMA((3,)),
        ],
        compiler_params=pltpu.CompilerParams(vmem_limit_bytes=14 * 1024 * 1024),
        cost_estimate=pl.CostEstimate(
            flops=6 * rows * D * width, bytes_accessed=6 * D * width, transcendentals=0
        ),
        name="project",
    )(*operands)


def attend_kernel(first, last, count, split, *refs):
    q_ref = refs[0]
    if split:
        pairs = [(refs[1], refs[2], 0)]
        refs = refs[3:]
    else:
        pairs = [(ref, ref, ref.shape[0] // 2) for ref in refs[1 : 1 + count]]
        refs = refs[1 + count :]
    key_rows = pairs[0][0].shape[0] - pairs[0][2]
    if not first:
        top_in, denom_in, acc_in = refs[:3]
        refs = refs[3:]
    heads = q_ref.shape[1] // HD
    scale = math.log2(math.e) * HD ** (-0.5)

    def attend_head(head, _):
        lanes = pl.ds(head * HD if last else pl.multiple_of(head * HD, HD), HD)
        query = q_ref[:, lanes]
        scores = [
            lax.dot_general(
                keys[:key_rows, lanes],
                query,
                (((1,), (1,)), ((), ())),
                preferred_element_type=jnp.float32,
            )
            for keys, _, _ in pairs
        ]
        top = functools.reduce(jnp.maximum, [jnp.max(s, axis=0, keepdims=True) for s in scores])
        if not first:
            top = jnp.maximum(top, top_in[head])
        shift = top * scale
        denom = None
        acc = None
        for score, (_, vals, offset) in zip(scores, pairs):
            expo = jnp.exp2(score * scale - shift)
            part = jnp.sum(expo, axis=0, keepdims=True)
            term = lax.dot_general(
                vals[offset : offset + key_rows, lanes],
                expo.astype(jnp.bfloat16),
                (((0,), (0,)), ((), ())),
                preferred_element_type=jnp.float32,
            )
            denom = part if denom is None else denom + part
            acc = term if acc is None else acc + term
        if not first:
            factor = jnp.exp2(top_in[head] * scale - shift)
            denom = denom + denom_in[head] * factor
            acc = acc + acc_in[head] * factor
        if last:
            refs[0][:, lanes] = (acc / denom).T.astype(jnp.bfloat16)
        else:
            refs[0][head] = top
            refs[1][head] = denom
            refs[2][head] = acc
        return 0

    if last:
        for head in range(heads):
            attend_head(head, 0)
    else:
        lax.fori_loop(0, heads, attend_head, 0)


def attend(queries, blocks, state, last):
    rows, width = queries.shape
    heads = width // HD
    key_rows = sum(block.shape[0] for block in blocks) // 2
    vmem = pl.BlockSpec(memory_space=pltpu.VMEM)
    row = jax.ShapeDtypeStruct((heads, 1, rows), jnp.float32)
    held = (row, row, jax.ShapeDtypeStruct((heads, HD, rows), jnp.float32))
    out_shape = jax.ShapeDtypeStruct((rows, width), jnp.bfloat16) if last else held
    first = state is None
    operands = [queries] + list(blocks) + ([] if first else list(state))
    return pl.pallas_call(
        functools.partial(attend_kernel, first, last, len(blocks), last),
        out_shape=out_shape,
        in_specs=[vmem] * len(operands),
        out_specs=vmem if last else (vmem,) * 3,
        compiler_params=pltpu.CompilerParams(vmem_limit_bytes=8 * 1024 * 1024),
        cost_estimate=pl.CostEstimate(
            flops=4 * rows * key_rows * width,
            bytes_accessed=4 * key_rows * width,
            transcendentals=rows * key_rows * heads,
        ),
        name="attend",
    )(*operands)


def finish_kernel(where, guidance, step_index, step_count, own_w, attn_ref, *refs):
    (
        own_hidden,
        other_hidden,
        own_vecs,
        other_vecs,
        b_out,
        w_final,
        b_final,
        latent,
        prev,
    ) = refs[:9]
    pieces = refs[9:-11]
    (
        next_out,
        denoised_out,
        w_ref,
        hidden_ref,
        vecs_ref,
        b_out_ref,
        w_final_ref,
        b_final_ref,
        latent_ref,
        prev_ref,
        sem,
    ) = refs[-11:]
    peers = 1 + w_ref.shape[0]
    half = pieces[0].shape[0]
    here, core = where[0], where[1]
    rows, channels = latent_ref.shape
    groups = []
    for shift in range(1, peers):
        group = []
        for index in range(2):
            part = core if index == 0 else 1 - core
            span = pl.ds(pl.multiple_of(part * half, half), half)
            group.append((pieces[2 * shift - 2 + index], w_ref.at[shift - 1, span]))
        groups.append(group)
    groups.append(
        [
            (own_hidden, hidden_ref.at[core]),
            (other_hidden, hidden_ref.at[1 - core]),
            (own_vecs, vecs_ref.at[core]),
            (other_vecs, vecs_ref.at[1 - core]),
            (b_out, b_out_ref),
            (w_final, w_final_ref),
            (b_final, b_final_ref),
            (latent, latent_ref),
            (prev, prev_ref),
        ]
    )
    copies = []
    at = 0
    for group in groups:
        copies.append([pltpu.make_async_copy(*p, sem.at[at + i]) for i, p in enumerate(group)])
        at += len(group)
    for group in copies:
        for copy in group:
            copy.start()

    def arrived(at):
        for copy in copies[at]:
            copy.wait()

    def of_both(at):
        return jnp.concatenate(
            [jnp.broadcast_to(vecs_ref[b, at : at + 1], (rows, D)) for b in range(2)], axis=0
        )

    index = jnp.full((1, channels), step_index[0], jnp.int32).astype(jnp.float32)
    count = jnp.full((1, channels), step_count[0], jnp.int32).astype(jnp.float32)
    sigma_prev = noise_level(index - 1.0, count)
    sigma_now = noise_level(index, count)
    sigma_next = noise_level(index + 1.0, count)
    step_now = log_ratio(sigma_next) - log_ratio(sigma_now)
    step_prev = log_ratio(sigma_now) - log_ratio(sigma_prev)
    ratio = step_prev / step_now
    fade = (1.0 - sigma_next) * (jnp.exp(-step_now) - 1.0)

    projected = None
    for shift in range(peers):
        source = lax.rem(here + peers - shift, peers)
        left = jnp.concatenate([attn_ref[b, source] for b in range(2)], axis=0)
        if shift > 0:
            arrived(shift - 1)
        weight = own_w[...] if shift == 0 else w_ref[shift - 1]
        term = jnp.dot(left, weight, preferred_element_type=jnp.float32)
        projected = term if projected is None else projected + term
    arrived(-1)
    hidden = hidden_ref[...].reshape(2 * rows, D).astype(jnp.float32)
    mixed = hidden + of_both(0) * (projected + b_out_ref[...])
    normed = layer_norm(mixed)
    final_in = (normed * (1.0 + of_both(2)) + of_both(1)).astype(jnp.bfloat16)
    velocity = (
        lax.dot_general(
            final_in, w_final_ref[...], (((1,), (1,)), ((), ())), preferred_element_type=jnp.float32
        )
        + b_final_ref[...]
    )
    cond = velocity[:rows]
    uncond = velocity[rows:]
    guided = uncond + guidance[0] * (cond - uncond)
    denoised = latent_ref[...] - sigma_now * guided
    blend = (1.0 + 0.5 / ratio) * denoised - 0.5 / ratio * prev_ref[...]
    denoised_out[...] = denoised
    next_out[...] = sigma_next / sigma_now * latent_ref[...] - fade * blend


def finish(scalars, own_w, attn, loaded, pieces):
    hidden, _, vecs, _, b_out, w_final, b_final, latent, prev = loaded
    rows, _ = latent.shape
    held = len(pieces) // 2
    depth = (1 + held) * own_w.shape[0]
    copies = len(loaded) + len(pieces)
    loaded = [pltpu.with_memory_space_constraint(x, pltpu.HBM) for x in (*loaded, *pieces)]
    hbm = pl.BlockSpec(memory_space=pltpu.HBM)
    vmem = pl.BlockSpec(memory_space=pltpu.VMEM)
    smem = pl.BlockSpec(memory_space=pltpu.SMEM)
    out = jax.ShapeDtypeStruct(latent.shape, jnp.float32)
    return pl.pallas_call(
        finish_kernel,
        out_shape=(out, out),
        in_specs=[smem] * len(scalars) + [vmem] * 2 + [hbm] * copies,
        out_specs=(vmem, vmem),
        scratch_shapes=[
            pltpu.VMEM((held,) + own_w.shape, own_w.dtype),
            pltpu.VMEM((2,) + hidden.shape, hidden.dtype),
            pltpu.VMEM((2,) + vecs.shape, vecs.dtype),
        ]
        + [pltpu.VMEM(x.shape, x.dtype) for x in (b_out, w_final, b_final, latent, prev)]
        + [pltpu.SemaphoreType.DMA((copies,))],
        compiler_params=pltpu.CompilerParams(vmem_limit_bytes=16 * 1024 * 1024),
        cost_estimate=pl.CostEstimate(
            flops=4 * rows * depth * D, bytes_accessed=2 * depth * D, transcendentals=0
        ),
        name="finish",
    )(*scalars, own_w, attn, *loaded)


def body(
    img_hidden,
    txt_hidden,
    modulation,
    w_qkv,
    q_gain,
    k_gain,
    w_out,
    b_out,
    stale_kv,
    final_mod,
    w_final,
    b_final,
    latent,
    prev_denoised,
    guidance,
    step_index,
    step_count,
):
    head_width = w_out.shape[0]
    img_rows = img_hidden.shape[1]
    txt_rows = txt_hidden.shape[1]
    kv_rows = img_rows + txt_rows
    out_rows = latent.shape[0]
    patch_index = lax.axis_index("patch")
    cfg_index = lax.axis_index("cfg")
    head_index = lax.axis_index("head")
    head_total = lax.axis_size("head")

    patches = lax.axis_size("patch")
    reach = patches // 2
    ahead = [(i, (i + 1) % patches) for i in range(patches)]
    back = [(i, (i - 1) % patches) for i in range(patches)]
    swap = [(0, 1), (1, 0)]
    hidden_rows = img_hidden.reshape(2, head_total, out_rows, D)
    hidden_mine = lax.dynamic_index_in_dim(hidden_rows, head_index, 1, keepdims=False)
    own_hidden = lax.dynamic_index_in_dim(hidden_mine, cfg_index, 0, keepdims=False)
    sent_hidden = lax.dynamic_index_in_dim(hidden_mine, 1 - cfg_index, 0, keepdims=False)
    own_vecs = jnp.concatenate([modulation[0, 2:], final_mod[0]], axis=0)
    gains = jnp.stack([q_gain, k_gain])
    stale = stale_kv.reshape(2 * kv_rows, head_width)
    rising = falling = stale
    arrived = []
    held = {}

    def work(step):
        if step == 1:
            held["w"] = (w_qkv[:, 0], w_qkv[:, 1], w_qkv[:, 2])
            held["turns"] = turn_tables(patch_index, img_rows, txt_rows)
            return (*held["w"], held["turns"])
        if step == 2:
            held["q"], held["fresh"] = project(
                txt_hidden[0], img_hidden[0], modulation[0, :2], *held["w"], gains, held["turns"]
            )
            return held["q"], held["fresh"]
        if step == 3:
            group = [held["fresh"].reshape(stale.shape)] + [x for p in arrived[:2] for x in p]
        else:
            group = list(arrived[step - 2])
        held["state"] = attend(held["q"], group, held.get("state"), False)
        return held["state"]

    for step in range(1, reach + 1):
        if step < reach:
            going = (rising, falling)
        else:
            going = (rising[:kv_rows], falling[kv_rows:])
        going = (lax.ppermute(going[0], "patch", ahead), lax.ppermute(going[1], "patch", back))
        made = work(step)
        arrived.append(going)
        if step < reach:
            if step == reach - 1:
                made = (*made, *sent)
            if step == reach - 2:
                other_hidden = lax.ppermute(sent_hidden, "cfg", swap)
                other_vecs = lax.ppermute(own_vecs, "cfg", swap)
                made = (*made, other_hidden, other_vecs)
            rising, falling, *tied = lax.optimization_barrier((*going, *made))
            if step == reach - 2:
                *tied, other_hidden, other_vecs = tied
            if step == reach - 1:
                sent = tied[-len(sent) :]
                tied = tied[: -len(sent)]
                pieces = [x for mine in sent for x in (mine, lax.ppermute(mine, "cfg", swap))]
            if step == 1:
                *held["w"], held["turns"] = tied
            elif step == 2:
                held["q"], held["fresh"] = tied
            else:
                held["state"] = tuple(tied)
            if step == 2:
                (w_tied,) = lax.optimization_barrier((w_out, rising))[:1]
                half = w_out.shape[0] // 2
                w_half = lax.dynamic_slice_in_dim(w_tied, cfg_index * half, half, 0)
                sent = []
                for shift in range(1, head_total):
                    ring = [(i, (i + shift) % head_total) for i in range(head_total)]
                    sent.append(lax.ppermute(w_half, "head", ring))
    fresh_kv = held["fresh"]
    attn = attend(held["q"], arrived[-1], held["state"], True)
    shared = lax.all_to_all(
        attn.reshape(2 * head_total, out_rows, head_width), ("cfg", "head"), 0, 0, tiled=True
    ).reshape(2, head_total, out_rows, head_width)
    where = jnp.stack([head_index, cfg_index])
    loaded = (
        own_hidden,
        other_hidden,
        own_vecs,
        other_vecs,
        b_out.reshape(1, D),
        w_final.T,
        b_final.reshape(1, CH),
        latent,
        prev_denoised,
    )
    next_latent, denoised = finish(
        (where, guidance, step_index, step_count), w_out, shared, loaded, pieces
    )
    return (fresh_kv[None], next_latent, denoised)


def solution(mesh):
    return jax.shard_map(
        body,
        mesh=mesh,
        in_specs=(
            P("cfg", ("groups", "patch"), None),
            P("cfg", ("groups", "patch"), None),
            P(("groups", "cfg"), None, None),
            P(None, None, "head"),
            P(),
            P(),
            P("head", None),
            P(),
            P("cfg", None, ("groups", "patch"), "head"),
            P(("groups", "cfg"), None, None),
            P(),
            P(),
            P(("groups", "patch", "cfg", "head"), None),
            P(("groups", "patch", "cfg", "head"), None),
            P("groups"),
            P(),
            P(),
        ),
        out_specs=(
            P("cfg", None, ("groups", "patch"), "head"),
            P(("groups", "patch", "cfg", "head"), None),
            P(("groups", "patch", "cfg", "head"), None),
        ),
        check_vma=False,
    )
```
